128 devices in a mesh: task: 2 (over z_lo), batch: 64 (over y, z_hi, x, core).
Axes of the slice: x: 4, y: 4, z: 4 (z_hi: 2, z_lo: 2; z = z_hi * 2 + z_lo), core: 2. Of those that a mesh axis runs over, the one named last changes fastest.
Arguments:
- pooled: bfloat16 [49152, 3328], P('batch'), may hold values from -6 to 6
- gate_weight: bfloat16 [3328, 8, 4], P(None, 'task'), may hold values from -0.21875 to 0.21875
- w_first: bfloat16 [8, 3328, 1024], P('task', 'batch'), may hold values from -0.15625 to 0.15625
- w_second: bfloat16 [8, 1024, 512], P('task', 'batch'), may hold values from -0.25 to 0.25
- w_third: bfloat16 [8, 512, 256], P('task', 'batch'), may hold values from -0.375 to 0.375
- tower_hidden: bfloat16 [4, 256, 128], P('task'), may hold values from -0.5 to 0.5
- tower_out: bfloat16 [4, 128], P('task'), may hold values from -0.75 to 0.75
Outputs:
- task_logits: float32 [49152, 4], P('batch', 'task')
The draws below stay inside these ranges and needn't reach their ends.
All inputs are finite; a program needn't handle non-finite values.
Results may differ from the reference program's by a relative error of at most 0.02.
Values may be sent and summed in bfloat16 or wider, within the bound.
A program may use at most 128 MiB of HBM per device.

```python
import jax
import jax.numpy as jnp

H1 = 1024
H2 = 512
H3 = 256
TOWER = 128
TASKS = 4
D_IN = 3328
EXPERTS = 8
TOKENS = 49152


def steps_of(own_key, extent, shards, smallest, largest):
    def one(position, parts):
        heights = jax.random.uniform(jax.random.fold_in(jax.random.fold_in(own_key, 6), position), (parts,), jnp.float32, smallest / len(shards), largest / len(shards))
        return jnp.repeat(jnp.exp(heights), extent[position] // parts).reshape((-1,) + (1,) * (len(extent) - position - 1))

    loudness = one(*shards[0])
    for cut in shards[1:]:
        loudness = loudness * one(*cut)
    return loudness


def centred(key, extent, width, limit, shards=(), kind=jnp.bfloat16):
    gain = steps_of(key, extent, shards, -0.22, 0.18) if shards else 1.0
    values = jax.random.normal(key, extent, jnp.float32) * width * gain
    return jnp.minimum(jnp.maximum(values, -limit), limit).astype(kind)


def setup_inputs(seed: int = 0) -> dict:
    streams_of = jax.random.split(jax.random.key(seed), 8)
    return {
        "pooled": centred(streams_of[0], (TOKENS, D_IN), 1.0, 6.0, ((0, 64),)),
        "gate_weight": centred(streams_of[1], (D_IN, EXPERTS, TASKS), (D_IN // 4) ** -0.5, 0.21875, ((1, 2),)),
        "w_first": centred(streams_of[2], (EXPERTS, D_IN, H1), (D_IN // 2) ** -0.5, 0.15625, ((0, 2), (1, 64))),
        "w_second": centred(streams_of[3], (EXPERTS, H1, H2), (H1 // 2) ** -0.5, 0.25, ((0, 2), (1, 64))),
        "w_third": centred(streams_of[4], (EXPERTS, H2, H3), (H2 // 2) ** -0.5, 0.375, ((0, 2), (1, 64))),
        "tower_hidden": centred(streams_of[5], (TASKS, H3, TOWER), (H3 // 2) ** -0.5, 0.5, ((0, 2),)),
        "tower_out": centred(streams_of[6], (TASKS, TOWER), (TOWER // 2) ** -0.5, 0.75, ((0, 2),)),
    }


def reference(pooled, gate_weight, w_first, w_second, w_third, tower_hidden, tower_out):
    logits = jnp.dot(pooled, gate_weight.reshape(D_IN, EXPERTS * TASKS), preferred_element_type=jnp.float32)
    logits = logits.reshape(TOKENS, EXPERTS, TASKS)
    weights = jnp.exp(logits)
    total = jnp.sum(weights, axis=1)
    numer = jnp.zeros((TOKENS, TASKS, H3), jnp.float32)
    for expert_id in range(EXPERTS):
        first = jax.nn.relu(jnp.dot(pooled, w_first[expert_id], preferred_element_type=jnp.float32)).astype(jnp.bfloat16)
        second = jax.nn.relu(jnp.dot(first, w_second[expert_id], preferred_element_type=jnp.float32)).astype(jnp.bfloat16)
        expert_out = jax.nn.relu(jnp.dot(second, w_third[expert_id], preferred_element_type=jnp.float32)).astype(jnp.bfloat16)
        numer = numer + weights[:, expert_id, :][:, :, None] * expert_out.astype(jnp.float32)[:, None, :]
    mix = (numer / total[:, :, None]).astype(jnp.bfloat16)
    tower = jax.nn.relu(jnp.einsum("sth,thk->stk", mix.astype(jnp.float32), tower_hidden.astype(jnp.float32))).astype(jnp.bfloat16)
    return jnp.einsum("stk,tk->st", tower.astype(jnp.float32), tower_out.astype(jnp.float32))
```

```python
import jax
import jax.numpy as jnp
from jax import lax
from jax.experimental import pallas as pl
from jax.experimental.pallas import tpu as pltpu
from jax.sharding import Mesh
from jax.sharding import PartitionSpec as P

AXES = ("task", "batch_0", "batch_1", "batch_2", "batch_3")
BATCH = AXES[1:]
MESH = pl.DeviceIdType.MESH
BF16 = jnp.bfloat16
F32 = jnp.float32

W1_ROWS, W2_ROWS, W3_ROWS = 52, 8, 4
QUAD = 4
BLOCK = W1_ROWS + W2_ROWS + W3_ROWS


def one_hot(rows, source):
    row = lax.broadcasted_iota(jnp.int32, (rows, QUAD * BLOCK), 0)
    column = lax.broadcasted_iota(jnp.int32, (rows, QUAD * BLOCK), 1)
    return jnp.where(source(row) == column, 1.0, 0.0).astype(BF16)


def picked(selector, values):
    return jnp.dot(selector, values, preferred_element_type=F32).astype(BF16)


def kernel(
    pooled_hbm, block_hbm, gate_hbm, hidden_ref, out_w_ref, out_ref,
    staged, w1, w23, pooled, gate, first, second, eo, numer, weights, send_sem, recv_sem, local_sem,
):
    t, y, zh, x, c = (lax.axis_index(a) for a in AXES)
    xp, xq = x // 2, lax.rem(x, 2)
    j = 2 * xq + c
    tq = jnp.where(zh == 1, t, 1 - t)
    experts = w1.shape[0]
    tokens = pooled.shape[0]

    def at(pos, k):
        return lax.rem(pos + (k + 4), 4)

    core_peer = (t, y, zh, x, 1 - c)
    z_peer = (1 - t, y, 1 - zh, x, c)
    task_peer = (1 - t, y, zh, x, c)
    x_dev = lambda k: (t, y, zh, at(x, k), c)
    y_dev = lambda k: (t, at(y, k), zh, x, c)

    def quad_dev(d):
        dx, dc = d // 2, d % 2
        return (tq, y, zh, 2 * xp + (1 - xq if dx else xq), 1 - c if dc else c)

    used = [0]
    sent = []

    def slot():
        used[0] += 1
        return used[0] - 1

    def push(i, src, dst, device):
        copy = pltpu.make_async_remote_copy(
            src_ref=src, dst_ref=dst, send_sem=send_sem.at[i], recv_sem=recv_sem.at[i],
            device_id=device, device_id_type=MESH,
        )
        copy.start()
        sent.append(copy)

    def arrived(i, dst):
        pltpu.make_async_remote_copy(
            src_ref=dst, dst_ref=dst, send_sem=send_sem.at[i], recv_sem=recv_sem.at[i],
            device_id=core_peer, device_id_type=MESH,
        ).wait_recv()

    half = tokens // 2
    loads = [
        pltpu.make_async_copy(pooled_hbm.at[pl.ds(k * half, half)], pooled.at[pl.ds(k * half, half)], local_sem.at[k])
        for k in range(2)
    ]
    loads.append(pltpu.make_async_copy(gate_hbm.at[t], gate.at[0], local_sem.at[2]))
    own_block = pltpu.make_async_copy(block_hbm.at[j], staged.at[j], local_sem.at[3])
    for load in loads:
        load.start()

    @pl.when(zh == 1)
    def _():
        own_block.start()

    barrier = pltpu.get_barrier_semaphore()
    peers = [x_dev(1), x_dev(-1), y_dev(1), y_dev(-1), z_peer, core_peer, task_peer] + [quad_dev(d) for d in range(1, QUAD)]
    for device in peers:
        pl.semaphore_signal(barrier, inc=1, device_id=device, device_id_type=MESH)
    pl.semaphore_wait(barrier, len(peers))

    quad_slots = [slot() for _ in range(QUAD)]
    for d in range(1, QUAD):
        to = 2 * ((1 - xq) if d // 2 else xq) + ((1 - c) if d % 2 else c)
        push(quad_slots[d], block_hbm.at[to], staged.at[j], quad_dev(d))
    own_far = pltpu.make_async_remote_copy(
        src_ref=block_hbm.at[j], dst_ref=staged.at[j], send_sem=send_sem.at[quad_slots[0]],
        recv_sem=recv_sem.at[quad_slots[0]], device_id=task_peer, device_id_type=MESH,
    )

    @pl.when(zh == 0)
    def _():
        own_far.start()

    gate_slot = slot()
    push(gate_slot, gate_hbm.at[1 - t], gate.at[1], task_peer)

    for d in range(1, QUAD):
        arrived(quad_slots[d], staged.at[2 * ((1 - xq) if d // 2 else xq) + ((1 - c) if d % 2 else c)])

    @pl.when(zh == 1)
    def _():
        own_block.wait()

    @pl.when(zh == 0)
    def _():
        own_far.wait()

    def w1_source(r):
        return r + (BLOCK - W1_ROWS) * (
            (r >= W1_ROWS).astype(jnp.int32) + (r >= 2 * W1_ROWS).astype(jnp.int32) + (r >= 3 * W1_ROWS).astype(jnp.int32)
        )

    def half_source(r, unit, side, base):
        member, within = r // (2 * unit), lax.rem(r, 2 * unit)
        return jnp.where(within // unit == side, BLOCK * member + base + lax.rem(within, unit), -1)

    pick1 = one_hot(QUAD * W1_ROWS, w1_source)
    pick2 = [one_hot(QUAD * 16, lambda r, s=s: half_source(r, W2_ROWS, s, W1_ROWS)) for s in range(2)]
    pick3 = [
        one_hot(16, lambda r, s=s: jnp.where(
            half_source(r, W3_ROWS, s, W1_ROWS + W2_ROWS) >= 0,
            half_source(r, W3_ROWS, s, W1_ROWS + W2_ROWS) + 2 * BLOCK * xq, -1))
        for s in range(2)
    ]
    col0 = pl.multiple_of(512 * c, 128)

    def w1_cols(h, xq_):
        return pl.ds(pl.multiple_of(512 * c + 256 * h + 128 * xq_, 128), 128)

    for e in range(experts):
        rows = staged[:, e].reshape(QUAD * BLOCK, 256)
        w1_part = picked(pick1, rows)
        w1[e, y, zh, xp, :, w1_cols(0, xq)] = w1_part[:, :128]
        w1[e, y, zh, xp, :, w1_cols(1, xq)] = w1_part[:, 128:]
        w23[e % 2, e // 2, y, zh, xp, xq, c, 0:64] = picked(
            jnp.concatenate(pick2, axis=1), jnp.concatenate([rows[:, :128], rows[:, 128:]], axis=0)
        )
        w23[e % 2, e // 2, y, zh, xp, xq, c, 64:80] = picked(
            jnp.concatenate(pick3, axis=1), jnp.concatenate([rows[:, :128], rows[:, 128:]], axis=0)
        )

    def plane(o):
        return zh if o == 0 else 1 - zh

    def a1(k, o):
        x_ = at(x, k)
        return w1.at[:, y, plane(o), x_ // 2, :, w1_cols(0, lax.rem(x_, 2))]

    def b1(k, o):
        return w1.at[:, at(y, k), plane(o), xp, :, w1_cols(1, xq)]

    def c1x(k, o):
        x_ = at(x, k)
        return w23.at[0, :, y, plane(o), x_ // 2, lax.rem(x_, 2), c]

    def c1y(k, o):
        return w23.at[1, :, at(y, k), plane(o), xp, xq, c]

    def a2(e, k, o, core):
        return w1.at[e, at(y, k), plane(o), :, :, pl.ds(pl.multiple_of(512 * core, 128), 256)]

    def b2(e, k, o, core):
        x_ = at(x, k)
        cols = pl.ds(pl.multiple_of(512 * core + 256 + 128 * lax.rem(x_, 2), 128), 128)
        return w1.at[e, :, plane(o), x_ // 2, :, cols]

    def c2(e, k, o, core):
        if e % 2 == 0:
            return w23.at[0, e // 2, at(y, k), plane(o), :, :, core]
        x_ = at(x, k)
        return w23.at[1, e // 2, :, plane(o), x_ // 2, lax.rem(x_, 2), core]

    class Ring:
        def __init__(self, device, part):
            self.device, self.part = device, part
            self.slots = {(o, k): slot() for o in range(2) for k in (1, -1, 2)}

        def near(self, o):
            for k in (1, -1):
                push(self.slots[o, k], self.part(0, o), self.part(0, o), self.device(k))

        def near_arrived(self, o):
            for k in (1, -1):
                arrived(self.slots[o, k], self.part(-k, o))

        def far(self, o):
            k = 1 if o == 0 else -1
            push(self.slots[o, 2], self.part(-k, o), self.part(-k, o), self.device(k))

        def far_arrived(self, o):
            arrived(self.slots[o, 2], self.part(2, o))

    one = [Ring(x_dev, a1), Ring(y_dev, b1), Ring(x_dev, c1x), Ring(y_dev, c1y)]
    two, shared = [], []
    for e in range(experts):
        parts = [
            (y_dev, lambda k, o, core=c, e=e: a2(e, k, o, core)),
            (x_dev, lambda k, o, core=c, e=e: b2(e, k, o, core)),
            (y_dev if e % 2 == 0 else x_dev, lambda k, o, core=c, e=e: c2(e, k, o, core)),
        ]
        two.append([Ring(device, part) for device, part in parts])
        shared.append([(part, {(k, o): slot() for k in (0, 1, -1, 2) for o in range(2)}) for _, part in parts])

    def share(e, which):
        for part, slots in shared[e]:
            for k in which:
                for o in range(2):
                    push(slots[k, o], part(k, o), part(k, o), core_peer)

    def share_arrived(e):
        for part, slots in shared[e]:
            for (k, o), i in slots.items():
                arrived(i, part(k, o, 1 - c))

    def each(rings, step, o):
        for ring in rings:
            getattr(ring, step)(o)

    z_slots = [slot() for _ in one]
    for ring, i in zip(one, z_slots):
        push(i, ring.part(0, 0), ring.part(0, 0), z_peer)
    each(one, "near", 0)

    for load in loads:
        load.wait()
    arrived(gate_slot, gate.at[1])
    own_gate = jnp.where(zh == 1, 0, 1)
    for o in range(2):
        g = gate[own_gate if o == 0 else 1 - own_gate]
        logits = lax.dot_general(pooled[...], g, (((1,), (1,)), ((), ())), preferred_element_type=F32)
        weights[o] = jnp.exp(logits)
    numer[...] = jnp.zeros_like(numer)

    each(one, "near_arrived", 0)
    each(one, "far", 0)
    each(one, "far_arrived", 0)
    each(two[0], "near", 0)
    for ring, i in zip(one, z_slots):
        arrived(i, ring.part(0, 1))
    each(one, "near", 1)
    each(one, "near_arrived", 1)
    each(one, "far", 1)
    each(one, "far_arrived", 1)
    each(two[0], "near", 1)
    for o in range(2):
        each(two[1], "near", o)

    eo_slots = [slot() for _ in range(experts)]
    assert used[0] <= send_sem.shape[0], used[0]

    def near_done(e):
        for o in range(2):
            each(two[e], "near_arrived", o)
            each(two[e], "far", o)
        share(e, (0, 1, -1))
        if e + 2 < experts:
            for o in range(2):
                each(two[e + 2], "near", o)

    def far_done(e):
        for o in range(2):
            each(two[e], "far_arrived", o)
        share(e, (2,))

    def add_up(o, e):
        values = eo[o, e].astype(F32)
        for k in range(2):
            numer[k] += weights[o, :, 2 * e + k : 2 * e + k + 1] * values

    def compute(e):
        @pl.loop(0, 4)
        def _(n):
            cols = pl.ds(pl.multiple_of(n * 256, 256), 256)
            w = w1[e, :, :, :, :, cols].reshape(16 * 208, 256)
            summed = jnp.dot(pooled[...], w, preferred_element_type=F32)
            first[:, cols] = jnp.maximum(summed, 0.0).astype(BF16)

        @pl.loop(0, 2)
        def _(n):
            cols = pl.ds(pl.multiple_of(n * 256, 256), 256)
            w = jnp.concatenate(
                [w23[e % 2, e // 2, :, :, :, q, n, 0:64].reshape(16 * 64, 128) for q in range(2)], axis=1
            )
            summed = jnp.dot(first[...], w, preferred_element_type=F32)
            second[:, cols] = jnp.maximum(summed, 0.0).astype(BF16)

        w = jnp.concatenate(
            [w23[e % 2, e // 2, :, :, :, :, n, 64:80].reshape(32 * 16, 128) for n in range(2)], axis=1
        )
        summed = jnp.dot(second[...], w, preferred_element_type=F32)
        eo[0, e] = jnp.maximum(summed, 0.0).astype(BF16)
        push(eo_slots[e], eo.at[0, e], eo.at[1, e], task_peer)
        add_up(0, e)

    near_done(0)
    near_done(1)
    far_done(0)
    for e in range(experts):
        share_arrived(e)
        compute(e)
        if e + 2 < experts:
            near_done(e + 2)
        if e + 1 < experts:
            far_done(e + 1)
    for e in range(experts):
        arrived(eo_slots[e], eo.at[1, e])
        add_up(1, e)

    for k in range(2):
        total = sum(weights[o, :, 2 * e + k : 2 * e + k + 1] for o in range(2) for e in range(experts))
        mix = (numer[k] / total).astype(BF16)
        tower = jnp.maximum(jnp.dot(mix, hidden_ref[k], preferred_element_type=F32), 0.0).astype(BF16)
        out_ref[:, k : k + 1] = jnp.sum(tower.astype(F32) * out_w_ref[k : k + 1, :].astype(F32), axis=1, keepdims=True)

    for copy in sent:
        copy.wait_send()


def per_device(pooled, gate_weight, w_first, w_second, w_third, tower_hidden, tower_out):
    tokens, width = pooled.shape
    experts = w_first.shape[0]
    one = w_first.reshape(experts, 52, 2, 2, 2, 128).transpose(4, 2, 0, 1, 3, 5).reshape(4, experts, 52, 256)
    two = w_second.reshape(experts, 2, 8, 2, 2, 128).transpose(4, 3, 0, 2, 1, 5).reshape(4, experts, 8, 256)
    three = w_third.reshape(experts, 2, 4, 2, 128).transpose(3, 0, 2, 1, 4).reshape(1, 2, experts, 4, 256)
    three = jnp.broadcast_to(three, (2, 2, experts, 4, 256)).reshape(4, experts, 4, 256)
    block = jnp.concatenate([one, two, three], axis=2)
    gate = gate_weight.reshape(width, experts, 2, 2).transpose(2, 1, 3, 0).reshape(2, 2 * experts, width)
    any_, vmem = pl.BlockSpec(memory_space=pl.ANY), pl.BlockSpec(memory_space=pltpu.VMEM)
    slots = 300
    return pl.pallas_call(
        kernel,
        out_shape=jax.ShapeDtypeStruct((tokens, 2), F32),
        in_specs=[any_, any_, any_, vmem, vmem],
        out_specs=vmem,
        scratch_shapes=[
            pltpu.VMEM((QUAD, experts, BLOCK, 256), BF16),
            pltpu.VMEM((experts, 4, 2, 2, 208, 1024), BF16),
            pltpu.VMEM((2, 2, 4, 2, 2, 2, 2, 80, 128), BF16),
            pltpu.VMEM((tokens, width), BF16),
            pltpu.VMEM((2, 2 * experts, width), BF16),
            pltpu.VMEM((tokens, 1024), BF16),
            pltpu.VMEM((tokens, 512), BF16),
            pltpu.VMEM((2, experts, tokens, 256), BF16),
            pltpu.VMEM((2, tokens, 256), F32),
            pltpu.VMEM((2, tokens, 2 * experts), F32),
            pltpu.SemaphoreType.DMA((slots,)),
            pltpu.SemaphoreType.DMA((slots,)),
            pltpu.SemaphoreType.DMA((4,)),
        ],
        compiler_params=pltpu.CompilerParams(
            collective_id=0, has_side_effects=True, vmem_limit_bytes=67_000_000
        ),
    )(pooled, block, gate, tower_hidden, tower_out)


def solution(mesh):
    torus = Mesh(mesh.devices.reshape(mesh.shape["task"], 4, 2, 4, 2), AXES)
    return jax.shard_map(
        per_device,
        mesh=torus,
        in_specs=(
            P(BATCH, None),
            P(None, "task", None),
            P("task", BATCH, None),
            P("task", BATCH, None),
            P("task", BATCH, None),
            P("task", None, None),
            P("task", None),
        ),
        out_specs=P(BATCH, "task"),
        check_vma=False,
    )
```

```python
import jax
import jax.numpy as jnp
from jax import lax
from jax.experimental import pallas as pl
from jax.experimental.pallas import tpu as pltpu
from jax.sharding import Mesh
from jax.sharding import PartitionSpec as P

AXES = ("task", "batch_0", "batch_1", "batch_2", "batch_3")
BATCH = AXES[1:]
MESH = pl.DeviceIdType.MESH
BF16 = jnp.bfloat16
F32 = jnp.float32

W1_ROWS, W2_ROWS, W3_ROWS = 52, 8, 4
QUAD = 4
BLOCK = W1_ROWS + W2_ROWS + W3_ROWS


def one_hot(rows, source):
    row = lax.broadcasted_iota(jnp.int32, (rows, QUAD * BLOCK), 0)
    column = lax.broadcasted_iota(jnp.int32, (rows, QUAD * BLOCK), 1)
    return jnp.where(source(row) == column, 1.0, 0.0).astype(BF16)


def picked(selector, values):
    return jnp.dot(selector, values, preferred_element_type=F32).astype(BF16)


def kernel(
    pooled_hbm, block_hbm, gate_hbm, hidden_ref, out_w_ref, out_ref,
    staged, w1, w23, pooled, gate, first, second, eo, numer, weights, send_sem, recv_sem, local_sem,
):
    t, y, zh, x, c = (lax.axis_index(a) for a in AXES)
    xp, xq = x // 2, lax.rem(x, 2)
    j = 2 * xq + c
    tq = jnp.where(zh == 1, t, 1 - t)
    experts = w1.shape[0]
    tokens = pooled.shape[0]

    def at(pos, k):
        return lax.rem(pos + (k + 4), 4)

    core_peer = (t, y, zh, x, 1 - c)
    z_peer = (1 - t, y, 1 - zh, x, c)
    task_peer = (1 - t, y, zh, x, c)
    x_dev = lambda k: (t, y, zh, at(x, k), c)
    y_dev = lambda k: (t, at(y, k), zh, x, c)

    def quad_dev(d):
        dx, dc = d // 2, d % 2
        return (tq, y, zh, 2 * xp + (1 - xq if dx else xq), 1 - c if dc else c)

    used = [0]
    sent = []

    def slot():
        used[0] += 1
        return used[0] - 1

    def push(i, src, dst, device):
        copy = pltpu.make_async_remote_copy(
            src_ref=src, dst_ref=dst, send_sem=send_sem.at[i], recv_sem=recv_sem.at[i],
            device_id=device, device_id_type=MESH,
        )
        copy.start()
        sent.append(copy)

    def arrived(i, dst):
        pltpu.make_async_remote_copy(
            src_ref=dst, dst_ref=dst, send_sem=send_sem.at[i], recv_sem=recv_sem.at[i],
            device_id=core_peer, device_id_type=MESH,
        ).wait_recv()

    half = tokens // 2
    loads = [
        pltpu.make_async_copy(pooled_hbm.at[pl.ds(k * half, half)], pooled.at[pl.ds(k * half, half)], local_sem.at[k])
        for k in range(2)
    ]
    loads.append(pltpu.make_async_copy(gate_hbm.at[t], gate.at[0], local_sem.at[2]))
    own_block = pltpu.make_async_copy(block_hbm.at[j], staged.at[j], local_sem.at[3])
    for load in loads:
        load.start()

    @pl.when(zh == 1)
    def _():
        own_block.start()

    barrier = pltpu.get_barrier_semaphore()
    peers = [x_dev(1), x_dev(-1), y_dev(1), y_dev(-1), z_peer, core_peer, task_peer] + [quad_dev(d) for d in range(1, QUAD)]
    for device in peers:
        pl.semaphore_signal(barrier, inc=1, device_id=device, device_id_type=MESH)
    pl.semaphore_wait(barrier, len(peers))

    def member(d):
        return 2 * ((1 - xq) if d // 2 else xq) + ((1 - c) if d % 2 else c)

    quad_slots = [[slot() for _ in range(QUAD)] for _ in range(experts)]
    own_far = []
    for e in range(experts):
        for d in range(1, QUAD):
            push(quad_slots[e][d], block_hbm.at[member(d), e], staged.at[j, e], quad_dev(d))
        own_far.append(pltpu.make_async_remote_copy(
            src_ref=block_hbm.at[j, e], dst_ref=staged.at[j, e], send_sem=send_sem.at[quad_slots[e][0]],
            recv_sem=recv_sem.at[quad_slots[e][0]], device_id=task_peer, device_id_type=MESH,
        ))

        @pl.when(zh == 0)
        def _(e=e):
            own_far[e].start()

    gate_slot = slot()
    push(gate_slot, gate_hbm.at[1 - t], gate.at[1], task_peer)

    @pl.when(zh == 1)
    def _():
        own_block.wait()

    def w1_source(r):
        return r + (BLOCK - W1_ROWS) * (
            (r >= W1_ROWS).astype(jnp.int32) + (r >= 2 * W1_ROWS).astype(jnp.int32) + (r >= 3 * W1_ROWS).astype(jnp.int32)
        )

    def half_source(r, unit, side, base):
        member, within = r // (2 * unit), lax.rem(r, 2 * unit)
        return jnp.where(within // unit == side, BLOCK * member + base + lax.rem(within, unit), -1)

    pick1 = one_hot(QUAD * W1_ROWS, w1_source)
    pick2 = [one_hot(QUAD * 16, lambda r, s=s: half_source(r, W2_ROWS, s, W1_ROWS)) for s in range(2)]
    pick3 = [
        one_hot(16, lambda r, s=s: jnp.where(
            half_source(r, W3_ROWS, s, W1_ROWS + W2_ROWS) >= 0,
            half_source(r, W3_ROWS, s, W1_ROWS + W2_ROWS) + 2 * BLOCK * xq, -1))
        for s in range(2)
    ]
    col0 = pl.multiple_of(512 * c, 128)

    def w1_cols(h, xq_):
        return pl.ds(pl.multiple_of(512 * c + 256 * h + 128 * xq_, 128), 128)

    def pack(e):
        for d in range(1, QUAD):
            arrived(quad_slots[e][d], staged.at[member(d), e])

        @pl.when(zh == 0)
        def _():
            own_far[e].wait()

        rows = staged[:, e].reshape(QUAD * BLOCK, 256)
        w1_part = picked(pick1, rows)
        w1[e, y, zh, xp, :, w1_cols(0, xq)] = w1_part[:, :128]
        w1[e, y, zh, xp, :, w1_cols(1, xq)] = w1_part[:, 128:]
        w23[e % 2, e // 2, y, zh, xp, xq, c, 0:64] = picked(
            jnp.concatenate(pick2, axis=1), jnp.concatenate([rows[:, :128], rows[:, 128:]], axis=0)
        )
        w23[e % 2, e // 2, y, zh, xp, xq, c, 64:80] = picked(
            jnp.concatenate(pick3, axis=1), jnp.concatenate([rows[:, :128], rows[:, 128:]], axis=0)
        )

    def plane(o):
        return zh if o == 0 else 1 - zh

    def a1(e, k):
        x_ = at(x, k)
        return w1.at[e, y, zh, x_ // 2, :, w1_cols(0, lax.rem(x_, 2))]

    def b1(e, k):
        return w1.at[e, at(y, k), zh, xp, :, w1_cols(1, xq)]

    def c1(e, k):
        if e % 2 == 0:
            x_ = at(x, k)
            return w23.at[0, e // 2, y, zh, x_ // 2, lax.rem(x_, 2), c]
        return w23.at[1, e // 2, at(y, k), zh, xp, xq, c]

    def a2(e, k, o, core):
        return w1.at[e, at(y, k), plane(o), :, :, pl.ds(pl.multiple_of(512 * core, 128), 256)]

    def b2(e, k, o, core):
        x_ = at(x, k)
        cols = pl.ds(pl.multiple_of(512 * core + 256 + 128 * lax.rem(x_, 2), 128), 128)
        return w1.at[e, :, plane(o), x_ // 2, :, cols]

    def c2(e, k, o, core):
        if e % 2 == 0:
            return w23.at[0, e // 2, at(y, k), plane(o), :, :, core]
        x_ = at(x, k)
        return w23.at[1, e // 2, :, plane(o), x_ // 2, lax.rem(x_, 2), core]

    class Ring:
        def __init__(self, device, part, way):
            self.device, self.part, self.way = device, part, way
            self.slots = {k: slot() for k in (1, -1, 2)}

        def near(self):
            for k in (1, -1):
                push(self.slots[k], self.part(0), self.part(0), self.device(k))

        def near_arrived(self):
            for k in (1, -1):
                arrived(self.slots[k], self.part(-k))

        def far(self):
            self.near_arrived()
            k = self.way
            push(self.slots[2], self.part(-k), self.part(-k), self.device(k))

        def far_arrived(self):
            arrived(self.slots[2], self.part(2))

    one, two, z_slots, shared = [], [], [], []
    for e in range(experts):
        third = y_dev if e % 2 == 0 else x_dev
        first_third = x_dev if e % 2 == 0 else y_dev
        parts = [
            (x_dev, lambda k, e=e: a1(e, k), y_dev, lambda k, o, core=c, e=e: a2(e, k, o, core)),
            (y_dev, lambda k, e=e: b1(e, k), x_dev, lambda k, o, core=c, e=e: b2(e, k, o, core)),
            (first_third, lambda k, e=e: c1(e, k), third, lambda k, o, core=c, e=e: c2(e, k, o, core)),
        ]
        one.append([Ring(d1, p1, 1 if (e + i) % 2 == 0 else -1) for i, (d1, p1, _, _) in enumerate(parts)])
        two.append([
            [Ring(d2, lambda k, p2=p2, o=o: p2(k, o), 1 if o == 0 else -1) for _, _, d2, p2 in parts] for o in range(2)
        ])
        z_slots.append([slot() for _ in parts])
        shared.append([(p2, {(k, o): slot() for k in (0, 1, -1, 2) for o in range(2)}) for _, _, _, p2 in parts])

    def share(e, o, which):
        for part, slots in shared[e]:
            for k in which:
                push(slots[k, o], part(k, o), part(k, o), core_peer)

    def share_arrived(e):
        for part, slots in shared[e]:
            for (k, o), i in slots.items():
                arrived(i, part(k, o, 1 - c))

    def each(rings, step):
        for ring in rings:
            getattr(ring, step)()

    def first_round(e):
        pack(e)
        each(one[e], "near")

    def first_far(e):
        each(one[e], "far")

    def first_done(e):
        each(one[e], "far_arrived")
        for (part, _), i in zip(shared[e], z_slots[e]):
            push(i, part(0, 0), part(0, 0), z_peer)

    def near(e, o):
        each(two[e][o], "near")

    def z_done(e):
        for (part, _), i in zip(shared[e], z_slots[e]):
            arrived(i, part(0, 1))
        near(e, 1)

    def far(e, o):
        each(two[e][o], "far")
        share(e, o, (0, 1, -1))

    def far_done(e):
        for o in range(2):
            each(two[e][o], "far_arrived")
            share(e, o, (2,))

    def gates():
        for load in loads:
            load.wait()
        arrived(gate_slot, gate.at[1])
        own_gate = jnp.where(zh == 1, 0, 1)
        for o in range(2):
            g = gate[own_gate if o == 0 else 1 - own_gate]
            logits = lax.dot_general(pooled[...], g, (((1,), (1,)), ((), ())), preferred_element_type=F32)
            weights[o] = jnp.exp(logits)
        numer[...] = jnp.zeros_like(numer)

    eo_slots = [slot() for _ in range(experts)]
    assert used[0] <= send_sem.shape[0], used[0]

    def add_up(o, e):
        values = eo[o, e].astype(F32)
        for k in range(2):
            numer[k] += weights[o, :, 2 * e + k : 2 * e + k + 1] * values

    def compute(e, between=None):
        for start in range(0, 4, 2):
            @pl.loop(start, start + 2)
            def _(n):
                cols = pl.ds(pl.multiple_of(n * 256, 256), 256)
                w = w1[e, :, :, :, :, cols].reshape(16 * 208, 256)
                summed = jnp.dot(pooled[...], w, preferred_element_type=F32)
                first[:, cols] = jnp.maximum(summed, 0.0).astype(BF16)

            if start == 0 and between is not None:
                between()

        @pl.loop(0, 2)
        def _(n):
            cols = pl.ds(pl.multiple_of(n * 256, 256), 256)
            w = jnp.concatenate(
                [w23[e % 2, e // 2, :, :, :, q, n, 0:64].reshape(16 * 64, 128) for q in range(2)], axis=1
            )
            summed = jnp.dot(first[...], w, preferred_element_type=F32)
            second[:, cols] = jnp.maximum(summed, 0.0).astype(BF16)

        w = jnp.concatenate(
            [w23[e % 2, e // 2, :, :, :, :, n, 64:80].reshape(32 * 16, 128) for n in range(2)], axis=1
        )
        summed = jnp.dot(second[...], w, preferred_element_type=F32)
        eo[0, e] = jnp.maximum(summed, 0.0).astype(BF16)
        push(eo_slots[e], eo.at[0, e], eo.at[1, e], task_peer)
        add_up(0, e)

    first_round(0)
    first_round(1)
    first_far(0)
    first_round(2)
    first_done(0)
    near(0, 0)
    first_far(1)
    first_round(3)
    first_done(1)
    near(1, 0)
    first_far(2)
    gates()
    z_done(0)
    far(0, 0)
    first_done(2)
    near(2, 0)
    first_far(3)
    far(0, 1)
    first_done(3)
    z_done(1)
    far(1, 0)
    far_done(0)
    near(3, 0)
    share_arrived(0)
    compute(0, lambda: far(1, 1))
    z_done(2)
    far(2, 0)
    far_done(1)
    share_arrived(1)
    compute(1, lambda: far(2, 1))
    z_done(3)
    far(3, 0)
    far_done(2)
    share_arrived(2)
    compute(2, lambda: far(3, 1))
    far_done(3)
    share_arrived(3)
    compute(3)
    for e in range(experts):
        arrived(eo_slots[e], eo.at[1, e])
        add_up(1, e)

    for k in range(2):
        total = sum(weights[o, :, 2 * e + k : 2 * e + k + 1] for o in range(2) for e in range(experts))
        mix = (numer[k] / total).astype(BF16)
        tower = jnp.maximum(jnp.dot(mix, hidden_ref[k], preferred_element_type=F32), 0.0).astype(BF16)
        out_ref[:, k : k + 1] = jnp.sum(tower.astype(F32) * out_w_ref[k : k + 1, :].astype(F32), axis=1, keepdims=True)

    for copy in sent:
        copy.wait_send()


def per_device(pooled, gate_weight, w_first, w_second, w_third, tower_hidden, tower_out):
    tokens, width = pooled.shape
    experts = w_first.shape[0]
    one = w_first.reshape(experts, 52, 2, 2, 2, 128).transpose(4, 2, 0, 1, 3, 5).reshape(4, experts, 52, 256)
    two = w_second.reshape(experts, 2, 8, 2, 2, 128).transpose(4, 3, 0, 2, 1, 5).reshape(4, experts, 8, 256)
    three = w_third.reshape(experts, 2, 4, 2, 128).transpose(3, 0, 2, 1, 4).reshape(1, 2, experts, 4, 256)
    three = jnp.broadcast_to(three, (2, 2, experts, 4, 256)).reshape(4, experts, 4, 256)
    block = jnp.concatenate([one, two, three], axis=2)
    gate = gate_weight.reshape(width, experts, 2, 2).transpose(2, 1, 3, 0).reshape(2, 2 * experts, width)
    any_, vmem = pl.BlockSpec(memory_space=pl.ANY), pl.BlockSpec(memory_space=pltpu.VMEM)
    slots = 300
    return pl.pallas_call(
        kernel,
        out_shape=jax.ShapeDtypeStruct((tokens, 2), F32),
        in_specs=[any_, any_, any_, vmem, vmem],
        out_specs=vmem,
        scratch_shapes=[
            pltpu.VMEM((QUAD, experts, BLOCK, 256), BF16),
            pltpu.VMEM((experts, 4, 2, 2, 208, 1024), BF16),
            pltpu.VMEM((2, 2, 4, 2, 2, 2, 2, 80, 128), BF16),
            pltpu.VMEM((tokens, width), BF16),
            pltpu.VMEM((2, 2 * experts, width), BF16),
            pltpu.VMEM((tokens, 1024), BF16),
            pltpu.VMEM((tokens, 512), BF16),
            pltpu.VMEM((2, experts, tokens, 256), BF16),
            pltpu.VMEM((2, tokens, 256), F32),
            pltpu.VMEM((2, tokens, 2 * experts), F32),
            pltpu.SemaphoreType.DMA((slots,)),
            pltpu.SemaphoreType.DMA((slots,)),
            pltpu.SemaphoreType.DMA((4,)),
        ],
        compiler_params=pltpu.CompilerParams(
            collective_id=0, has_side_effects=True, vmem_limit_bytes=67_000_000
        ),
    )(pooled, block, gate, tower_hidden, tower_out)


def solution(mesh):
    torus = Mesh(mesh.devices.reshape(mesh.shape["task"], 4, 2, 4, 2), AXES)
    return jax.shard_map(
        per_device,
        mesh=torus,
        in_specs=(
            P(BATCH, None),
            P(None, "task", None),
            P("task", BATCH, None),
            P("task", BATCH, None),
            P("task", BATCH, None),
            P("task", None, None),
            P("task", None),
        ),
        out_specs=P(BATCH, "task"),
        check_vma=False,
    )
```

```python
import functools

import jax
import jax.numpy as jnp
from jax import lax
from jax.experimental import pallas as pl
from jax.experimental.pallas import tpu as pltpu
from jax.sharding import Mesh
from jax.sharding import PartitionSpec as P

AXES = ("task", "batch_0", "batch_1", "batch_2", "batch_3")
BATCH = AXES[1:]
MESH = pl.DeviceIdType.MESH
BF16 = jnp.bfloat16
F32 = jnp.float32

W1_ROWS, W2_ROWS, W3_ROWS = 52, 8, 4
QUAD = 4
BLOCK = W1_ROWS + W2_ROWS + W3_ROWS


def one_hot(rows, source):
    row = lax.broadcasted_iota(jnp.int32, (rows, QUAD * BLOCK), 0)
    column = lax.broadcasted_iota(jnp.int32, (rows, QUAD * BLOCK), 1)
    return jnp.where(source(row) == column, 1.0, 0.0).astype(BF16)


def picked(selector, values):
    return jnp.dot(selector, values, preferred_element_type=F32).astype(BF16)


def kernel(
    pooled_hbm, block_hbm, gate_hbm, hidden_ref, out_w_ref, out_ref,
    staged, w1, w23, pooled, gate, first, second, eo, numer, weights, send_sem, recv_sem, local_sem,
):
    t, y, zh, x, c = (lax.axis_index(a) for a in AXES)
    xp, xq = x // 2, lax.rem(x, 2)
    j = 2 * xq + c
    tq = jnp.where(zh == 1, t, 1 - t)
    experts = w1.shape[0]
    tokens = pooled.shape[0]

    def at(pos, k):
        return lax.rem(pos + (k + 4), 4)

    core_peer = (t, y, zh, x, 1 - c)
    z_peer = (1 - t, y, 1 - zh, x, c)
    task_peer = (1 - t, y, zh, x, c)
    x_dev = lambda k: (t, y, zh, at(x, k), c)
    y_dev = lambda k: (t, at(y, k), zh, x, c)

    def quad_dev(d):
        dx, dc = d // 2, d % 2
        return (tq, y, zh, 2 * xp + (1 - xq if dx else xq), 1 - c if dc else c)

    used = [0]
    sent = []

    def slot():
        used[0] += 1
        return used[0] - 1

    def push(i, src, dst, device):
        copy = pltpu.make_async_remote_copy(
            src_ref=src, dst_ref=dst, send_sem=send_sem.at[i], recv_sem=recv_sem.at[i],
            device_id=device, device_id_type=MESH,
        )
        copy.start()
        sent.append(copy)

    def arrived(i, dst):
        pltpu.make_async_remote_copy(
            src_ref=dst, dst_ref=dst, send_sem=send_sem.at[i], recv_sem=recv_sem.at[i],
            device_id=core_peer, device_id_type=MESH,
        ).wait_recv()

    half = tokens // 2
    loads = [
        pltpu.make_async_copy(pooled_hbm.at[pl.ds(k * half, half)], pooled.at[pl.ds(k * half, half)], local_sem.at[k])
        for k in range(2)
    ]
    loads.append(pltpu.make_async_copy(gate_hbm.at[t], gate.at[0], local_sem.at[2]))
    own_block = pltpu.make_async_copy(block_hbm.at[j], staged.at[j], local_sem.at[3])
    for load in loads:
        load.start()

    @pl.when(zh == 1)
    def _():
        own_block.start()

    barrier = pltpu.get_barrier_semaphore()
    peers = [x_dev(1), x_dev(-1), y_dev(1), y_dev(-1), z_peer, core_peer, task_peer] + [quad_dev(d) for d in range(1, QUAD)]
    for device in peers:
        pl.semaphore_signal(barrier, inc=1, device_id=device, device_id_type=MESH)
    pl.semaphore_wait(barrier, len(peers))

    def member(d):
        return 2 * ((1 - xq) if d // 2 else xq) + ((1 - c) if d % 2 else c)

    quad_slots = [[slot() for _ in range(QUAD)] for _ in range(experts)]
    own_far = [
        pltpu.make_async_remote_copy(
            src_ref=block_hbm.at[j, e], dst_ref=staged.at[j, e], send_sem=send_sem.at[quad_slots[e][0]],
            recv_sem=recv_sem.at[quad_slots[e][0]], device_id=task_peer, device_id_type=MESH,
        )
        for e in range(experts)
    ]

    def quad(e):
        for d in range(1, QUAD):
            push(quad_slots[e][d], block_hbm.at[member(d), e], staged.at[j, e], quad_dev(d))

        @pl.when(zh == 0)
        def _():
            own_far[e].start()

    quad(0)

    gate_slot = slot()

    @pl.when(zh == 1)
    def _():
        own_block.wait()

    def w1_source(r):
        return r + (BLOCK - W1_ROWS) * (
            (r >= W1_ROWS).astype(jnp.int32) + (r >= 2 * W1_ROWS).astype(jnp.int32) + (r >= 3 * W1_ROWS).astype(jnp.int32)
        )

    def half_source(r, unit, side, base):
        member, within = r // (2 * unit), lax.rem(r, 2 * unit)
        return jnp.where(within // unit == side, BLOCK * member + base + lax.rem(within, unit), -1)

    pick1 = one_hot(QUAD * W1_ROWS, w1_source)
    pick2 = [one_hot(QUAD * 16, lambda r, s=s: half_source(r, W2_ROWS, s, W1_ROWS)) for s in range(2)]
    pick3 = [
        one_hot(16, lambda r, s=s: jnp.where(
            half_source(r, W3_ROWS, s, W1_ROWS + W2_ROWS) >= 0,
            half_source(r, W3_ROWS, s, W1_ROWS + W2_ROWS) + 2 * BLOCK * xq, -1))
        for s in range(2)
    ]
    col0 = pl.multiple_of(512 * c, 128)

    def w1_cols(h, xq_):
        return pl.ds(pl.multiple_of(512 * c + 256 * h + 128 * xq_, 128), 128)

    def pack(e):
        for d in range(1, QUAD):
            arrived(quad_slots[e][d], staged.at[member(d), e])

        @pl.when(zh == 0)
        def _():
            own_far[e].wait()

        rows = staged[:, e].reshape(QUAD * BLOCK, 256)
        w1_part = picked(pick1, rows)
        w1[e, y, zh, xp, :, w1_cols(0, xq)] = w1_part[:, :128]
        w1[e, y, zh, xp, :, w1_cols(1, xq)] = w1_part[:, 128:]
        w23[e % 2, e // 2, y, zh, xp, xq, c, 0:64] = picked(
            jnp.concatenate(pick2, axis=1), jnp.concatenate([rows[:, :128], rows[:, 128:]], axis=0)
        )
        w23[e % 2, e // 2, y, zh, xp, xq, c, 64:80] = picked(
            jnp.concatenate(pick3, axis=1), jnp.concatenate([rows[:, :128], rows[:, 128:]], axis=0)
        )

    def plane(o):
        return zh if o == 0 else 1 - zh

    def a1(e, k):
        x_ = at(x, k)
        return w1.at[e, y, zh, x_ // 2, :, w1_cols(0, lax.rem(x_, 2))]

    def b1(e, k):
        return w1.at[e, at(y, k), zh, xp, :, w1_cols(1, xq)]

    def c1(e, k):
        if e % 2 == 0:
            x_ = at(x, k)
            return w23.at[0, e // 2, y, zh, x_ // 2, lax.rem(x_, 2), c]
        return w23.at[1, e // 2, at(y, k), zh, xp, xq, c]

    def a2(e, k, o, core, rows=slice(None)):
        return w1.at[e, at(y, k), plane(o), rows, :, pl.ds(pl.multiple_of(512 * core, 128), 256)]

    def b2(e, k, o, core, rows=slice(None)):
        x_ = at(x, k)
        cols = pl.ds(pl.multiple_of(512 * core + 256 + 128 * lax.rem(x_, 2), 128), 128)
        return w1.at[e, rows, plane(o), x_ // 2, :, cols]

    def c2(e, k, o, core, rows=slice(None)):
        if e % 2 == 0:
            return w23.at[0, e // 2, at(y, k), plane(o), rows, :, core]
        x_ = at(x, k)
        return w23.at[1, e // 2, rows, plane(o), x_ // 2, lax.rem(x_, 2), core]

    class Ring:
        def __init__(self, device, part, ways):
            self.device, self.part, self.ways = device, part, ways
            self.slots = {k: slot() for k in (1, -1)}
            self.far_slots = {k: slot() for k in ways}

        def near(self):
            for k in (1, -1):
                push(self.slots[k], self.part(0), self.part(0), self.device(k))

        def far(self):
            for k in (1, -1):
                arrived(self.slots[k], self.part(-k))
            for k, half in self.ways.items():
                push(self.far_slots[k], half(-k), half(-k), self.device(k))

        def far_arrived(self):
            for k, half in self.ways.items():
                arrived(self.far_slots[k], half(2))

    one, two, z_slots, shared = [], [], [], []
    for e in range(experts):
        x_first, y_first = (x_dev, y_dev), (y_dev, x_dev)
        parts = [
            (x_first, lambda k, e=e: a1(e, k), functools.partial(a2, e), 2),
            (y_first, lambda k, e=e: b1(e, k), functools.partial(b2, e), 4),
            (x_first if e % 2 == 0 else y_first, lambda k, e=e: c1(e, k), functools.partial(c2, e), 2 if e % 2 == 0 else 4),
        ]
        one.append([Ring(d[0], p1, {(1 if (e + i) % 2 == 0 else -1): p1}) for i, (d, p1, _, _) in enumerate(parts)])
        two.append([
            [
                Ring(d[1], lambda k, p2=p2, o=o: p2(k, o, c), {
                    1: lambda k, p2=p2, o=o, n=n: p2(k, o, c, pl.ds(0, n // 2)),
                    -1: lambda k, p2=p2, o=o, n=n: p2(k, o, c, pl.ds(n // 2, n // 2)),
                })
                for d, _, p2, n in parts
            ]
            for o in range(2)
        ])
        z_slots.append([slot() for _ in parts])
        shared.append([(p2, {(k, o): slot() for k in (0, 1, -1, 2) for o in range(2)}) for _, _, p2, _ in parts])

    def share(e, o, which):
        for part, slots in shared[e]:
            for k in which:
                push(slots[k, o], part(k, o, c), part(k, o, c), core_peer)

    def share_arrived(e):
        for part, slots in shared[e]:
            for (k, o), i in slots.items():
                arrived(i, part(k, o, 1 - c))

    def each(rings, step):
        for ring in rings:
            getattr(ring, step)()

    def first_round(e):
        pack(e)
        each(one[e], "near")

    def first_far(e):
        each(one[e], "far")

    def first_done(e):
        each(one[e], "far_arrived")
        for (part, _), i in zip(shared[e], z_slots[e]):
            push(i, part(0, 0, c), part(0, 0, c), z_peer)

    def near(e, o):
        each(two[e][o], "near")

    def z_done(e):
        for (part, _), i in zip(shared[e], z_slots[e]):
            arrived(i, part(0, 1, c))
        near(e, 1)

    def far(e, o):
        each(two[e][o], "far")
        share(e, o, (0, 1, -1))

    def far_done(e):
        for o in range(2):
            each(two[e][o], "far_arrived")
            share(e, o, (2,))

    def gates():
        for load in loads:
            load.wait()
        arrived(gate_slot, gate.at[1])
        own_gate = jnp.where(zh == 1, 0, 1)
        for o in range(2):
            g = gate[own_gate if o == 0 else 1 - own_gate]
            logits = lax.dot_general(pooled[...], g, (((1,), (1,)), ((), ())), preferred_element_type=F32)
            weights[o] = jnp.exp(logits)
        numer[...] = jnp.zeros_like(numer)

    chunk = tokens // 3
    eo_slots = [slot() for _ in range(experts - 1)]
    last_slots = [slot() for _ in range(3)]
    assert used[0] <= send_sem.shape[0], used[0]

    def add_up(o, e, rows=slice(None)):
        values = eo[o, e, rows].astype(F32)
        for k in range(2):
            numer[k, rows] += weights[o, rows, 2 * e + k : 2 * e + k + 1] * values

    def layer_one(e, start, stop, rows=slice(None)):
        @pl.loop(start, stop)
        def _(n):
            cols = pl.ds(pl.multiple_of(n * 256, 256), 256)
            w = w1[e, :, :, :, :, cols].reshape(16 * 208, 256)
            summed = jnp.dot(pooled[rows], w, preferred_element_type=F32)
            first[rows, cols] = jnp.maximum(summed, 0.0).astype(BF16)

    def layers_two_three(e, rows=slice(None)):
        @pl.loop(0, 2)
        def _(n):
            cols = pl.ds(pl.multiple_of(n * 256, 256), 256)
            w = jnp.concatenate(
                [w23[e % 2, e // 2, :, :, :, q, n, 0:64].reshape(16 * 64, 128) for q in range(2)], axis=1
            )
            summed = jnp.dot(first[rows], w, preferred_element_type=F32)
            second[rows, cols] = jnp.maximum(summed, 0.0).astype(BF16)

        w = jnp.concatenate(
            [w23[e % 2, e // 2, :, :, :, :, n, 64:80].reshape(32 * 16, 128) for n in range(2)], axis=1
        )
        summed = jnp.dot(second[rows], w, preferred_element_type=F32)
        eo[0, e, rows] = jnp.maximum(summed, 0.0).astype(BF16)

    def compute(e, *between):
        layer_one(e, 0, 2)
        if between:
            between[0]()
        layer_one(e, 2, 4)
        if len(between) > 1:
            between[1]()
        layers_two_three(e)
        push(eo_slots[e], eo.at[0, e], eo.at[1, e], task_peer)
        add_up(0, e)

    def compute_last(e):
        for i in range(3):
            rows = pl.ds(i * chunk, chunk)
            layer_one(e, 0, 4, rows)
            layers_two_three(e, rows)
            push(last_slots[i], eo.at[0, e, rows], eo.at[1, e, rows], task_peer)
            add_up(0, e, rows)

    def finish(i):
        rows = pl.ds(i * chunk, chunk)
        arrived(last_slots[i], eo.at[1, experts - 1, rows])
        add_up(1, experts - 1, rows)
        for k in range(2):
            total = sum(weights[o, rows, 2 * e + k : 2 * e + k + 1] for o in range(2) for e in range(experts))
            mix = (numer[k, rows] / total).astype(BF16)
            tower = jnp.maximum(jnp.dot(mix, hidden_ref[k], preferred_element_type=F32), 0.0).astype(BF16)
            products = tower.astype(F32) * out_w_ref[k : k + 1, :].astype(F32)
            out_ref[rows, k : k + 1] = jnp.sum(products, axis=1, keepdims=True)

    def others(e):
        arrived(eo_slots[e], eo.at[1, e])
        add_up(1, e)

    first_round(0)
    quad(1)
    quad(2)
    quad(3)
    push(gate_slot, gate_hbm.at[1 - t], gate.at[1], task_peer)
    first_far(0)
    first_done(0)
    near(0, 0)
    first_round(1)
    first_round(2)
    first_round(3)
    gates()
    first_far(1)
    first_far(2)
    first_far(3)
    first_done(1)
    near(1, 0)
    z_done(0)
    first_done(2)
    far(0, 0)
    first_done(3)
    near(2, 0)
    far(0, 1)
    z_done(1)
    far(1, 0)
    near(3, 0)
    far_done(0)
    share_arrived(0)
    compute(0, lambda: far(1, 1), lambda: z_done(2))
    far(2, 0)
    far_done(1)
    share_arrived(1)
    compute(1, lambda: far(2, 1), lambda: z_done(3))
    far(3, 0)
    others(0)
    far_done(2)
    share_arrived(2)
    compute(2, lambda: far(3, 1))
    others(1)
    far_done(3)
    share_arrived(3)
    compute_last(3)
    others(2)
    for i in range(3):
        finish(i)

    for copy in sent:
        copy.wait_send()


def per_device(pooled, gate_weight, w_first, w_second, w_third, tower_hidden, tower_out):
    tokens, width = pooled.shape
    experts = w_first.shape[0]
    one = w_first.reshape(experts, 52, 2, 2, 2, 128).transpose(4, 2, 0, 1, 3, 5).reshape(4, experts, 52, 256)
    two = w_second.reshape(experts, 2, 8, 2, 2, 128).transpose(4, 3, 0, 2, 1, 5).reshape(4, experts, 8, 256)
    three = w_third.reshape(experts, 2, 4, 2, 128).transpose(3, 0, 2, 1, 4).reshape(1, 2, experts, 4, 256)
    three = jnp.broadcast_to(three, (2, 2, experts, 4, 256)).reshape(4, experts, 4, 256)
    block = jnp.concatenate([one, two, three], axis=2)
    gate = gate_weight.reshape(width, experts, 2, 2).transpose(2, 1, 3, 0).reshape(2, 2 * experts, width)
    any_, vmem = pl.BlockSpec(memory_space=pl.ANY), pl.BlockSpec(memory_space=pltpu.VMEM)
    slots = 300
    return pl.pallas_call(
        kernel,
        out_shape=jax.ShapeDtypeStruct((tokens, 2), F32),
        in_specs=[any_, any_, any_, vmem, vmem],
        out_specs=vmem,
        scratch_shapes=[
            pltpu.VMEM((QUAD, experts, BLOCK, 256), BF16),
            pltpu.VMEM((experts, 4, 2, 2, 208, 1024), BF16),
            pltpu.VMEM((2, 2, 4, 2, 2, 2, 2, 80, 128), BF16),
            pltpu.VMEM((tokens, width), BF16),
            pltpu.VMEM((2, 2 * experts, width), BF16),
            pltpu.VMEM((tokens, 1024), BF16),
            pltpu.VMEM((tokens, 512), BF16),
            pltpu.VMEM((2, experts, tokens, 256), BF16),
            pltpu.VMEM((2, tokens, 256), F32),
            pltpu.VMEM((2, tokens, 2 * experts), F32),
            pltpu.SemaphoreType.DMA((slots,)),
            pltpu.SemaphoreType.DMA((slots,)),
            pltpu.SemaphoreType.DMA((4,)),
        ],
        compiler_params=pltpu.CompilerParams(
            collective_id=0, has_side_effects=True, vmem_limit_bytes=67_000_000
        ),
    )(pooled, block, gate, tower_hidden, tower_out)


def solution(mesh):
    torus = Mesh(mesh.devices.reshape(mesh.shape["task"], 4, 2, 4, 2), AXES)
    return jax.shard_map(
        per_device,
        mesh=torus,
        in_specs=(
            P(BATCH, None),
            P(None, "task", None),
            P("task", BATCH, None),
            P("task", BATCH, None),
            P("task", BATCH, None),
            P("task", None, None),
            P("task", None),
        ),
        out_specs=P(BATCH, "task"),
        check_vma=False,
    )
```

```python
import functools

import jax
import jax.numpy as jnp
from jax import lax
from jax.experimental import pallas as pl
from jax.experimental.pallas import tpu as pltpu
from jax.sharding import Mesh
from jax.sharding import PartitionSpec as P

AXES = ("task", "batch_0", "batch_1", "batch_2", "batch_3")
BATCH = AXES[1:]
MESH = pl.DeviceIdType.MESH
BF16 = jnp.bfloat16
F32 = jnp.float32

W1_ROWS, W2_ROWS, W3_ROWS = 52, 8, 4
QUAD = 4
BLOCK = W1_ROWS + W2_ROWS + W3_ROWS


def one_hot(rows, source):
    row = lax.broadcasted_iota(jnp.int32, (rows, QUAD * BLOCK), 0)
    column = lax.broadcasted_iota(jnp.int32, (rows, QUAD * BLOCK), 1)
    return jnp.where(source(row) == column, 1.0, 0.0).astype(BF16)


def picked(selector, values):
    return jnp.dot(selector, values, preferred_element_type=F32).astype(BF16)


def kernel(
    pooled_hbm, gate_hbm, first_hbm, second_hbm, third_hbm, hidden_ref, out_w_ref, out_ref,
    raw1, raw2, raw3, block, staged, w1, w23, pooled, gate, first, second, eo, numer, weights, send_sem, recv_sem, local_sem,
):
    t, y, zh, x, c = (lax.axis_index(a) for a in AXES)
    xp, xq = x // 2, lax.rem(x, 2)
    j = 2 * xq + c
    tq = jnp.where(zh == 1, t, 1 - t)
    experts = w1.shape[0]
    tokens = pooled.shape[0]

    def at(pos, k):
        return lax.rem(pos + (k + 4), 4)

    core_peer = (t, y, zh, x, 1 - c)
    z_peer = (1 - t, y, 1 - zh, x, c)
    task_peer = (1 - t, y, zh, x, c)
    x_dev = lambda k: (t, y, zh, at(x, k), c)
    y_dev = lambda k: (t, at(y, k), zh, x, c)

    def quad_dev(d):
        dx, dc = d // 2, d % 2
        return (tq, y, zh, 2 * xp + (1 - xq if dx else xq), 1 - c if dc else c)

    used = [0]
    sent = []

    def slot():
        used[0] += 1
        return used[0] - 1

    def push(i, src, dst, device):
        copy = pltpu.make_async_remote_copy(
            src_ref=src, dst_ref=dst, send_sem=send_sem.at[i], recv_sem=recv_sem.at[i],
            device_id=device, device_id_type=MESH,
        )
        copy.start()
        sent.append(copy)

    def arrived(i, dst):
        pltpu.make_async_remote_copy(
            src_ref=dst, dst_ref=dst, send_sem=send_sem.at[i], recv_sem=recv_sem.at[i],
            device_id=core_peer, device_id_type=MESH,
        ).wait_recv()

    half = tokens // 2
    shards = [
        pltpu.make_async_copy(src, dst, local_sem.at[i])
        for i, (src, dst) in enumerate([(first_hbm, raw1), (second_hbm, raw2), (third_hbm, raw3)])
    ]
    loads = [
        pltpu.make_async_copy(pooled_hbm.at[pl.ds(k * half, half)], pooled.at[pl.ds(k * half, half)], local_sem.at[3 + k])
        for k in range(2)
    ]
    loads.append(pltpu.make_async_copy(gate_hbm, gate.at[0], local_sem.at[5]))
    for load in shards + loads:
        load.start()

    barrier = pltpu.get_barrier_semaphore()
    peers = [x_dev(1), x_dev(-1), y_dev(1), y_dev(-1), z_peer, core_peer, task_peer] + [quad_dev(d) for d in range(1, QUAD)]
    for device in peers:
        pl.semaphore_signal(barrier, inc=1, device_id=device, device_id_type=MESH)

    for load in shards:
        load.wait()

    def place(rows, columns, source):
        row = lax.broadcasted_iota(jnp.int32, (rows, columns), 0)
        column = lax.broadcasted_iota(jnp.int32, (rows, columns), 1)
        return jnp.where(source(row) == column, 1.0, 0.0).astype(BF16)

    def band(row, start, size, source):
        return jnp.where((row >= start) & (row < start + size), source, -1)

    def build(e):
        put1 = place(BLOCK, experts * W1_ROWS, lambda r: band(r, 0, W1_ROWS, experts * r + e))
        rows1 = jnp.dot(put1, raw1[...].reshape(experts * W1_ROWS, 1024), preferred_element_type=F32)
        rows2, rows3 = [], []
        for side in range(2):
            put2 = place(BLOCK, 16, lambda r: band(r, W1_ROWS, W2_ROWS, r - W1_ROWS + W2_ROWS * side))
            put3 = place(BLOCK, 8, lambda r: band(r, W1_ROWS + W2_ROWS, W3_ROWS, r - W1_ROWS - W2_ROWS + W3_ROWS * side))
            rows2.append(jnp.dot(put2, raw2[e], preferred_element_type=F32))
            rows3.append(jnp.dot(put3, raw3[e], preferred_element_type=F32))
        for member in range(QUAD):
            q, n = member // 2, member % 2
            for side in range(2):
                col1, col2, col3 = 512 * n + 256 * side + 128 * q, 256 * n + 128 * q, 128 * n
                both = rows1[:, col1 : col1 + 128] + rows2[side][:, col2 : col2 + 128] + rows3[side][:, col3 : col3 + 128]
                block[member, e, :, 128 * side : 128 * side + 128] = both.astype(BF16)

    build(0)
    pl.semaphore_wait(barrier, len(peers))

    def member(d):
        return 2 * ((1 - xq) if d // 2 else xq) + ((1 - c) if d % 2 else c)

    quad_slots = [[slot() for _ in range(QUAD)] for _ in range(experts)]
    own_far = [
        pltpu.make_async_remote_copy(
            src_ref=block.at[j, e], dst_ref=staged.at[j, e], send_sem=send_sem.at[quad_slots[e][0]],
            recv_sem=recv_sem.at[quad_slots[e][0]], device_id=task_peer, device_id_type=MESH,
        )
        for e in range(experts)
    ]

    def quad(e):
        for d in range(1, QUAD):
            push(quad_slots[e][d], block.at[member(d), e], staged.at[j, e], quad_dev(d))

        @pl.when(zh == 0)
        def _():
            own_far[e].start()

        @pl.when(zh == 1)
        def _():
            staged[j, e] = block[j, e]

    quad(0)
    for e in range(1, experts):
        build(e)
    gate_slot = slot()

    def w1_source(r):
        return r + (BLOCK - W1_ROWS) * (
            (r >= W1_ROWS).astype(jnp.int32) + (r >= 2 * W1_ROWS).astype(jnp.int32) + (r >= 3 * W1_ROWS).astype(jnp.int32)
        )

    def half_source(r, unit, side, base):
        member, within = r // (2 * unit), lax.rem(r, 2 * unit)
        return jnp.where(within // unit == side, BLOCK * member + base + lax.rem(within, unit), -1)

    pick1 = one_hot(QUAD * W1_ROWS, w1_source)
    pick2 = [one_hot(QUAD * 16, lambda r, s=s: half_source(r, W2_ROWS, s, W1_ROWS)) for s in range(2)]
    pick3 = [
        one_hot(16, lambda r, s=s: jnp.where(
            half_source(r, W3_ROWS, s, W1_ROWS + W2_ROWS) >= 0,
            half_source(r, W3_ROWS, s, W1_ROWS + W2_ROWS) + 2 * BLOCK * xq, -1))
        for s in range(2)
    ]
    col0 = pl.multiple_of(512 * c, 128)

    def w1_cols(h, xq_):
        return pl.ds(pl.multiple_of(512 * c + 256 * h + 128 * xq_, 128), 128)

    def pack(e):
        for d in range(1, QUAD):
            arrived(quad_slots[e][d], staged.at[member(d), e])

        @pl.when(zh == 0)
        def _():
            own_far[e].wait()

        rows = staged[:, e].reshape(QUAD * BLOCK, 256)
        w1_part = picked(pick1, rows)
        w1[e, y, zh, xp, :, w1_cols(0, xq)] = w1_part[:, :128]
        w1[e, y, zh, xp, :, w1_cols(1, xq)] = w1_part[:, 128:]
        w23[e % 2, e // 2, y, zh, xp, xq, c, 0:64] = picked(
            jnp.concatenate(pick2, axis=1), jnp.concatenate([rows[:, :128], rows[:, 128:]], axis=0)
        )
        w23[e % 2, e // 2, y, zh, xp, xq, c, 64:80] = picked(
            jnp.concatenate(pick3, axis=1), jnp.concatenate([rows[:, :128], rows[:, 128:]], axis=0)
        )

    def plane(o):
        return zh if o == 0 else 1 - zh

    def a1(e, k):
        x_ = at(x, k)
        return w1.at[e, y, zh, x_ // 2, :, w1_cols(0, lax.rem(x_, 2))]

    def b1(e, k):
        return w1.at[e, at(y, k), zh, xp, :, w1_cols(1, xq)]

    def c1(e, k):
        if e % 2 == 0:
            x_ = at(x, k)
            return w23.at[0, e // 2, y, zh, x_ // 2, lax.rem(x_, 2), c]
        return w23.at[1, e // 2, at(y, k), zh, xp, xq, c]

    def a2(e, k, o, core, rows=slice(None)):
        return w1.at[e, at(y, k), plane(o), rows, :, pl.ds(pl.multiple_of(512 * core, 128), 256)]

    def b2(e, k, o, core, rows=slice(None)):
        x_ = at(x, k)
        cols = pl.ds(pl.multiple_of(512 * core + 256 + 128 * lax.rem(x_, 2), 128), 128)
        return w1.at[e, rows, plane(o), x_ // 2, :, cols]

    def c2(e, k, o, core, rows=slice(None)):
        if e % 2 == 0:
            return w23.at[0, e // 2, at(y, k), plane(o), rows, :, core]
        x_ = at(x, k)
        return w23.at[1, e // 2, rows, plane(o), x_ // 2, lax.rem(x_, 2), core]

    class Ring:
        def __init__(self, device, part, ways):
            self.device, self.part, self.ways = device, part, ways
            self.slots = {k: slot() for k in (1, -1)}
            self.far_slots = {k: slot() for k in ways}

        def near(self):
            for k in (1, -1):
                push(self.slots[k], self.part(0), self.part(0), self.device(k))

        def far(self):
            for k in (1, -1):
                arrived(self.slots[k], self.part(-k))
            for k, half in self.ways.items():
                push(self.far_slots[k], half(-k), half(-k), self.device(k))

        def far_arrived(self):
            for k, half in self.ways.items():
                arrived(self.far_slots[k], half(2))

    one, two, z_slots, shared = [], [], [], []
    for e in range(experts):
        x_first, y_first = (x_dev, y_dev), (y_dev, x_dev)
        parts = [
            (x_first, lambda k, e=e: a1(e, k), functools.partial(a2, e), 2),
            (y_first, lambda k, e=e: b1(e, k), functools.partial(b2, e), 4),
            (x_first if e % 2 == 0 else y_first, lambda k, e=e: c1(e, k), functools.partial(c2, e), 2 if e % 2 == 0 else 4),
        ]
        one.append([Ring(d[0], p1, {(1 if (e + i) % 2 == 0 else -1): p1}) for i, (d, p1, _, _) in enumerate(parts)])
        two.append([
            [
                Ring(d[1], lambda k, p2=p2, o=o: p2(k, o, c), {
                    1: lambda k, p2=p2, o=o, n=n: p2(k, o, c, pl.ds(0, n // 2)),
                    -1: lambda k, p2=p2, o=o, n=n: p2(k, o, c, pl.ds(n // 2, n // 2)),
                })
                for d, _, p2, n in parts
            ]
            for o in range(2)
        ])
        z_slots.append([slot() for _ in parts])
        shared.append([(p2, {(k, o): slot() for k in (0, 1, -1, 2) for o in range(2)}) for _, _, p2, _ in parts])

    def share(e, o, which):
        for part, slots in shared[e]:
            for k in which:
                push(slots[k, o], part(k, o, c), part(k, o, c), core_peer)

    def share_arrived(e):
        for part, slots in shared[e]:
            for (k, o), i in slots.items():
                arrived(i, part(k, o, 1 - c))

    def each(rings, step):
        for ring in rings:
            getattr(ring, step)()

    def first_round(e):
        pack(e)
        each(one[e], "near")

    def first_far(e):
        each(one[e], "far")

    def first_done(e):
        each(one[e], "far_arrived")
        for (part, _), i in zip(shared[e], z_slots[e]):
            push(i, part(0, 0, c), part(0, 0, c), z_peer)

    def near(e, o):
        each(two[e][o], "near")

    def z_done(e):
        for (part, _), i in zip(shared[e], z_slots[e]):
            arrived(i, part(0, 1, c))
        near(e, 1)

    def far(e, o):
        each(two[e][o], "far")
        share(e, o, (0, 1, -1))

    def far_done(e):
        for o in range(2):
            each(two[e][o], "far_arrived")
            share(e, o, (2,))

    def gates():
        for load in loads:
            load.wait()
        arrived(gate_slot, gate.at[1])
        own_gate = jnp.where(zh == 1, 0, 1)
        for o in range(2):
            g = gate[own_gate if o == 0 else 1 - own_gate].reshape(4 * experts, pooled.shape[1])
            logits = lax.dot_general(pooled[...], g, (((1,), (1,)), ((), ())), preferred_element_type=F32)
            for e in range(experts):
                own = jnp.where(t == 0, logits[:, 4 * e : 4 * e + 2], logits[:, 4 * e + 2 : 4 * e + 4])
                weights[o, :, 2 * e : 2 * e + 2] = jnp.exp(own)
        numer[...] = jnp.zeros_like(numer)

    chunk = tokens // 3
    eo_slots = [slot() for _ in range(experts - 1)]
    last_slots = [slot() for _ in range(3)]
    assert used[0] <= send_sem.shape[0], used[0]

    def add_up(o, e, rows=slice(None)):
        values = eo[o, e, rows].astype(F32)
        for k in range(2):
            numer[k, rows] += weights[o, rows, 2 * e + k : 2 * e + k + 1] * values

    def layer_one(e, start, stop, rows=slice(None)):
        @pl.loop(start, stop)
        def _(n):
            cols = pl.ds(pl.multiple_of(n * 256, 256), 256)
            w = w1[e, :, :, :, :, cols].reshape(16 * 208, 256)
            summed = jnp.dot(pooled[rows], w, preferred_element_type=F32)
            first[rows, cols] = jnp.maximum(summed, 0.0).astype(BF16)

    def layers_two_three(e, rows=slice(None)):
        @pl.loop(0, 2)
        def _(n):
            cols = pl.ds(pl.multiple_of(n * 256, 256), 256)
            w = jnp.concatenate(
                [w23[e % 2, e // 2, :, :, :, q, n, 0:64].reshape(16 * 64, 128) for q in range(2)], axis=1
            )
            summed = jnp.dot(first[rows], w, preferred_element_type=F32)
            second[rows, cols] = jnp.maximum(summed, 0.0).astype(BF16)

        w = jnp.concatenate(
            [w23[e % 2, e // 2, :, :, :, :, n, 64:80].reshape(32 * 16, 128) for n in range(2)], axis=1
        )
        summed = jnp.dot(second[rows], w, preferred_element_type=F32)
        eo[0, e, rows] = jnp.maximum(summed, 0.0).astype(BF16)

    def compute(e, *between):
        layer_one(e, 0, 2)
        if between:
            between[0]()
        layer_one(e, 2, 4)
        if len(between) > 1:
            between[1]()
        layers_two_three(e)
        push(eo_slots[e], eo.at[0, e], eo.at[1, e], task_peer)
        add_up(0, e)

    def compute_last(e):
        for i in range(3):
            rows = pl.ds(i * chunk, chunk)
            layer_one(e, 0, 4, rows)
            layers_two_three(e, rows)
            push(last_slots[i], eo.at[0, e, rows], eo.at[1, e, rows], task_peer)
            add_up(0, e, rows)

    def finish(i):
        rows = pl.ds(i * chunk, chunk)
        arrived(last_slots[i], eo.at[1, experts - 1, rows])
        add_up(1, experts - 1, rows)
        for k in range(2):
            total = sum(weights[o, rows, 2 * e + k : 2 * e + k + 1] for o in range(2) for e in range(experts))
            mix = (numer[k, rows] / total).astype(BF16)
            tower = jnp.maximum(jnp.dot(mix, hidden_ref[k], preferred_element_type=F32), 0.0).astype(BF16)
            out_ref[k : k + 1, rows] = lax.dot_general(
                out_w_ref[k : k + 1, :], tower, (((1,), (1,)), ((), ())), preferred_element_type=F32
            )

    def others(e):
        arrived(eo_slots[e], eo.at[1, e])
        add_up(1, e)

    first_round(0)
    quad(1)
    quad(2)
    quad(3)
    push(gate_slot, gate_hbm, gate.at[1], task_peer)
    first_far(0)
    first_done(0)
    near(0, 0)
    first_round(1)
    first_round(2)
    first_round(3)
    gates()
    first_far(1)
    first_far(2)
    first_far(3)
    first_done(1)
    near(1, 0)
    z_done(0)
    first_done(2)
    far(0, 0)
    first_done(3)
    near(2, 0)
    far(0, 1)
    z_done(1)
    far(1, 0)
    near(3, 0)
    far_done(0)
    share_arrived(0)
    compute(0, lambda: far(1, 1), lambda: z_done(2))
    far(2, 0)
    far_done(1)
    share_arrived(1)
    compute(1, lambda: far(2, 1), lambda: z_done(3))
    far(3, 0)
    others(0)
    far_done(2)
    share_arrived(2)
    compute(2, lambda: far(3, 1))
    others(1)
    far_done(3)
    share_arrived(3)
    compute_last(3)
    others(2)
    for i in range(3):
        finish(i)

    for copy in sent:
        copy.wait_send()


def per_device(pooled, gate_weight, w_first, w_second, w_third, tower_hidden, tower_out):
    tokens, width = pooled.shape
    experts = w_first.shape[0]
    any_, vmem = pl.BlockSpec(memory_space=pl.ANY), pl.BlockSpec(memory_space=pltpu.VMEM)
    slots = 300
    return pl.pallas_call(
        kernel,
        out_shape=jax.ShapeDtypeStruct((2, tokens), F32),
        in_specs=[any_] * 5 + [vmem, vmem],
        out_specs=vmem,
        scratch_shapes=[
            pltpu.VMEM((52, experts, 1024), BF16),
            pltpu.VMEM((experts, 16, 512), BF16),
            pltpu.VMEM((experts, 8, 256), BF16),
            pltpu.VMEM((QUAD, experts, BLOCK, 256), BF16),
            pltpu.VMEM((QUAD, experts, BLOCK, 256), BF16),
            pltpu.VMEM((experts, 4, 2, 2, 208, 1024), BF16),
            pltpu.VMEM((2, 2, 4, 2, 2, 2, 2, 80, 128), BF16),
            pltpu.VMEM((tokens, width), BF16),
            pltpu.VMEM((2, experts, 4, width), BF16),
            pltpu.VMEM((tokens, 1024), BF16),
            pltpu.VMEM((tokens, 512), BF16),
            pltpu.VMEM((2, experts, tokens, 256), BF16),
            pltpu.VMEM((2, tokens, 256), F32),
            pltpu.VMEM((2, tokens, 2 * experts), F32),
            pltpu.SemaphoreType.DMA((slots,)),
            pltpu.SemaphoreType.DMA((slots,)),
            pltpu.SemaphoreType.DMA((6,)),
        ],
        compiler_params=pltpu.CompilerParams(
            collective_id=0, has_side_effects=True, vmem_limit_bytes=67_000_000
        ),
    )(
        pooled, gate_weight.transpose(1, 2, 0), w_first.transpose(1, 0, 2), w_second, w_third, tower_hidden, tower_out
    ).T


def solution(mesh):
    torus = Mesh(mesh.devices.reshape(mesh.shape["task"], 4, 2, 4, 2), AXES)
    return jax.shard_map(
        per_device,
        mesh=torus,
        in_specs=(
            P(BATCH, None),
            P(None, "task", None),
            P("task", BATCH, None),
            P("task", BATCH, None),
            P("task", BATCH, None),
            P("task", None, None),
            P("task", None),
        ),
        out_specs=P(BATCH, "task"),
        check_vma=False,
    )
```

```python
import functools

import jax
import jax.numpy as jnp
from jax import lax
from jax.experimental import pallas as pl
from jax.experimental.pallas import tpu as pltpu
from jax.sharding import Mesh
from jax.sharding import PartitionSpec as P

AXES = ("task", "batch_0", "batch_1", "batch_2", "batch_3")
BATCH = AXES[1:]
MESH = pl.DeviceIdType.MESH
BF16 = jnp.bfloat16
F32 = jnp.float32

W1_ROWS, W2_ROWS, W3_ROWS = 52, 8, 4
QUAD = 4
BLOCK = W1_ROWS + W2_ROWS + W3_ROWS


def one_hot(rows, source):
    row = lax.broadcasted_iota(jnp.int32, (rows, QUAD * BLOCK), 0)
    column = lax.broadcasted_iota(jnp.int32, (rows, QUAD * BLOCK), 1)
    return jnp.where(source(row) == column, 1.0, 0.0).astype(BF16)


def picked(selector, values):
    return jnp.dot(selector, values, preferred_element_type=F32).astype(BF16)


def kernel(
    pooled_hbm, gate_hbm, first_hbm, second_hbm, third_hbm, hidden_ref, out_w_ref, out_ref,
    raw1, raw2, raw3, block, staged, w1, w23, pooled, gate, first, second, eo, numer, weights, send_sem, recv_sem, local_sem,
):
    t, y, zh, x, c = (lax.axis_index(a) for a in AXES)
    xp, xq = x // 2, lax.rem(x, 2)
    j = 2 * xq + c
    tq = jnp.where(zh == 1, t, 1 - t)
    experts = w1.shape[0]
    tokens = pooled.shape[0]

    def at(pos, k):
        return lax.rem(pos + (k + 4), 4)

    core_peer = (t, y, zh, x, 1 - c)
    z_peer = (1 - t, y, 1 - zh, x, c)
    task_peer = (1 - t, y, zh, x, c)
    x_dev = lambda k: (t, y, zh, at(x, k), c)
    y_dev = lambda k: (t, at(y, k), zh, x, c)

    def quad_dev(d):
        dx, dc = d // 2, d % 2
        return (tq, y, zh, 2 * xp + (1 - xq if dx else xq), 1 - c if dc else c)

    used = [0]
    sent = []

    def slot():
        used[0] += 1
        return used[0] - 1

    def push(i, src, dst, device):
        copy = pltpu.make_async_remote_copy(
            src_ref=src, dst_ref=dst, send_sem=send_sem.at[i], recv_sem=recv_sem.at[i],
            device_id=device, device_id_type=MESH,
        )
        copy.start()
        sent.append(copy)

    def arrived(i, dst):
        pltpu.make_async_remote_copy(
            src_ref=dst, dst_ref=dst, send_sem=send_sem.at[i], recv_sem=recv_sem.at[i],
            device_id=core_peer, device_id_type=MESH,
        ).wait_recv()

    half = tokens // 2
    shards = [
        pltpu.make_async_copy(src, dst, local_sem.at[i])
        for i, (src, dst) in enumerate([(first_hbm, raw1), (second_hbm, raw2), (third_hbm, raw3)])
    ]
    loads = [
        pltpu.make_async_copy(pooled_hbm.at[pl.ds(k * half, half)], pooled.at[pl.ds(k * half, half)], local_sem.at[3 + k])
        for k in range(2)
    ]
    loads.append(pltpu.make_async_copy(gate_hbm, gate.at[0], local_sem.at[5]))
    for load in shards + loads:
        load.start()

    barrier = pltpu.get_barrier_semaphore()
    peers = [x_dev(1), x_dev(-1), x_dev(2), y_dev(1), y_dev(-1), y_dev(2), z_peer, core_peer, task_peer] + [quad_dev(d) for d in range(1, QUAD)]
    for device in peers:
        pl.semaphore_signal(barrier, inc=1, device_id=device, device_id_type=MESH)

    for load in shards:
        load.wait()

    def place(rows, columns, source):
        row = lax.broadcasted_iota(jnp.int32, (rows, columns), 0)
        column = lax.broadcasted_iota(jnp.int32, (rows, columns), 1)
        return jnp.where(source(row) == column, 1.0, 0.0).astype(BF16)

    def band(row, start, size, source):
        return jnp.where((row >= start) & (row < start + size), source, -1)

    def build(e):
        put1 = place(BLOCK, experts * W1_ROWS, lambda r: band(r, 0, W1_ROWS, experts * r + e))
        rows1 = jnp.dot(put1, raw1[...].reshape(experts * W1_ROWS, 1024), preferred_element_type=F32)
        rows2, rows3 = [], []
        for side in range(2):
            put2 = place(BLOCK, 16, lambda r: band(r, W1_ROWS, W2_ROWS, r - W1_ROWS + W2_ROWS * side))
            put3 = place(BLOCK, 8, lambda r: band(r, W1_ROWS + W2_ROWS, W3_ROWS, r - W1_ROWS - W2_ROWS + W3_ROWS * side))
            rows2.append(jnp.dot(put2, raw2[e], preferred_element_type=F32))
            rows3.append(jnp.dot(put3, raw3[e], preferred_element_type=F32))
        for member in range(QUAD):
            q, n = member // 2, member % 2
            for side in range(2):
                col1, col2, col3 = 512 * n + 256 * side + 128 * q, 256 * n + 128 * q, 128 * n
                both = rows1[:, col1 : col1 + 128] + rows2[side][:, col2 : col2 + 128] + rows3[side][:, col3 : col3 + 128]
                block[member, e, :, 128 * side : 128 * side + 128] = both.astype(BF16)

    build(0)
    pl.semaphore_wait(barrier, len(peers))

    def member(d):
        return 2 * ((1 - xq) if d // 2 else xq) + ((1 - c) if d % 2 else c)

    quad_slots = [[slot() for _ in range(QUAD)] for _ in range(experts)]
    own_far = [
        pltpu.make_async_remote_copy(
            src_ref=block.at[j, e], dst_ref=staged.at[j, e], send_sem=send_sem.at[quad_slots[e][0]],
            recv_sem=recv_sem.at[quad_slots[e][0]], device_id=task_peer, device_id_type=MESH,
        )
        for e in range(experts)
    ]

    def quad(e):
        for d in range(1, QUAD):
            push(quad_slots[e][d], block.at[member(d), e], staged.at[j, e], quad_dev(d))

        @pl.when(zh == 0)
        def _():
            own_far[e].start()

        @pl.when(zh == 1)
        def _():
            staged[j, e] = block[j, e]

    quad(0)
    for e in range(1, experts):
        build(e)
    gate_slot = slot()

    def w1_source(r):
        return r + (BLOCK - W1_ROWS) * (
            (r >= W1_ROWS).astype(jnp.int32) + (r >= 2 * W1_ROWS).astype(jnp.int32) + (r >= 3 * W1_ROWS).astype(jnp.int32)
        )

    def half_source(r, unit, side, base):
        member, within = r // (2 * unit), lax.rem(r, 2 * unit)
        return jnp.where(within // unit == side, BLOCK * member + base + lax.rem(within, unit), -1)

    pick1 = one_hot(QUAD * W1_ROWS, w1_source)
    pick2 = [one_hot(QUAD * 16, lambda r, s=s: half_source(r, W2_ROWS, s, W1_ROWS)) for s in range(2)]
    pick3 = [
        one_hot(16, lambda r, s=s: jnp.where(
            half_source(r, W3_ROWS, s, W1_ROWS + W2_ROWS) >= 0,
            half_source(r, W3_ROWS, s, W1_ROWS + W2_ROWS) + 2 * BLOCK * xq, -1))
        for s in range(2)
    ]
    col0 = pl.multiple_of(512 * c, 128)

    def w1_cols(h, xq_):
        return pl.ds(pl.multiple_of(512 * c + 256 * h + 128 * xq_, 128), 128)

    def pack(e):
        for d in range(1, QUAD):
            arrived(quad_slots[e][d], staged.at[member(d), e])

        @pl.when(zh == 0)
        def _():
            own_far[e].wait()

        rows = staged[:, e].reshape(QUAD * BLOCK, 256)
        w1_part = picked(pick1, rows)
        w1[e, y, zh, xp, :, w1_cols(0, xq)] = w1_part[:, :128]
        w1[e, y, zh, xp, :, w1_cols(1, xq)] = w1_part[:, 128:]
        w23[e % 2, e // 2, y, zh, xp, xq, c, 0:64] = picked(
            jnp.concatenate(pick2, axis=1), jnp.concatenate([rows[:, :128], rows[:, 128:]], axis=0)
        )
        w23[e % 2, e // 2, y, zh, xp, xq, c, 64:80] = picked(
            jnp.concatenate(pick3, axis=1), jnp.concatenate([rows[:, :128], rows[:, 128:]], axis=0)
        )

    def plane(o):
        return zh if o == 0 else 1 - zh

    def a1(e, k):
        x_ = at(x, k)
        return w1.at[e, y, zh, x_ // 2, :, w1_cols(0, lax.rem(x_, 2))]

    def b1(e, k):
        return w1.at[e, at(y, k), zh, xp, :, w1_cols(1, xq)]

    def c1(e, k):
        if e % 2 == 0:
            x_ = at(x, k)
            return w23.at[0, e // 2, y, zh, x_ // 2, lax.rem(x_, 2), c]
        return w23.at[1, e // 2, at(y, k), zh, xp, xq, c]

    def a2(e, k, o, core, rows=slice(None)):
        return w1.at[e, at(y, k), plane(o), rows, :, pl.ds(pl.multiple_of(512 * core, 128), 256)]

    def b2(e, k, o, core, rows=slice(None)):
        x_ = at(x, k)
        cols = pl.ds(pl.multiple_of(512 * core + 256 + 128 * lax.rem(x_, 2), 128), 128)
        return w1.at[e, rows, plane(o), x_ // 2, :, cols]

    def c2(e, k, o, core, rows=slice(None)):
        if e % 2 == 0:
            return w23.at[0, e // 2, at(y, k), plane(o), rows, :, core]
        x_ = at(x, k)
        return w23.at[1, e // 2, rows, plane(o), x_ // 2, lax.rem(x_, 2), core]

    class Ring:
        def __init__(self, device, part, ways, direct=False):
            self.device, self.part, self.ways, self.direct = device, part, ways, direct
            self.slots = {k: slot() for k in (1, -1)}
            self.far_slots = {k: slot() for k in ways}

        def near(self):
            for k in (1, -1):
                push(self.slots[k], self.part(0), self.part(0), self.device(k))
            if self.direct:
                for k in self.ways:
                    push(self.far_slots[k], self.part(0), self.part(0), self.device(2))

        def near_arrived(self):
            for k in (1, -1):
                arrived(self.slots[k], self.part(-k))

        def far(self):
            self.near_arrived()
            for k, half in self.ways.items():
                push(self.far_slots[k], half(-k), half(-k), self.device(k))

        def far_arrived(self):
            for k, half in self.ways.items():
                arrived(self.far_slots[k], half(2))

    one, two, z_slots, shared = [], [], [], []
    for e in range(experts):
        x_first, y_first = (x_dev, y_dev), (y_dev, x_dev)
        parts = [
            (x_first, lambda k, e=e: a1(e, k), functools.partial(a2, e), 2),
            (y_first, lambda k, e=e: b1(e, k), functools.partial(b2, e), 4),
            (x_first if e % 2 == 0 else y_first, lambda k, e=e: c1(e, k), functools.partial(c2, e), 2 if e % 2 == 0 else 4),
        ]
        one.append([Ring(d[0], p1, {(1 if (e + i) % 2 == 0 else -1): p1}, e < 1) for i, (d, p1, _, _) in enumerate(parts)])
        two.append([
            [
                Ring(d[1], lambda k, p2=p2, o=o: p2(k, o, c), {
                    1: lambda k, p2=p2, o=o, n=n: p2(k, o, c, pl.ds(0, n // 2)),
                    -1: lambda k, p2=p2, o=o, n=n: p2(k, o, c, pl.ds(n // 2, n // 2)),
                })
                for d, _, p2, n in parts
            ]
            for o in range(2)
        ])
        z_slots.append([slot() for _ in parts])
        shared.append([(p2, {(k, o): slot() for k in (0, 1, -1, 2) for o in range(2)}) for _, _, p2, _ in parts])

    def share(e, o, which):
        for part, slots in shared[e]:
            for k in which:
                push(slots[k, o], part(k, o, c), part(k, o, c), core_peer)

    def share_arrived(e):
        for part, slots in shared[e]:
            for (k, o), i in slots.items():
                arrived(i, part(k, o, 1 - c))

    def each(rings, step):
        for ring in rings:
            getattr(ring, step)()

    def first_round(e):
        pack(e)
        each(one[e], "near")

    def first_far(e):
        each(one[e], "far")

    def first_done(e):
        if e < 1:
            each(one[e], "near_arrived")
        each(one[e], "far_arrived")
        for (part, _), i in zip(shared[e], z_slots[e]):
            push(i, part(0, 0, c), part(0, 0, c), z_peer)

    def near(e, o):
        each(two[e][o], "near")

    def z_done(e):
        for (part, _), i in zip(shared[e], z_slots[e]):
            arrived(i, part(0, 1, c))
        near(e, 1)

    far_by_z = {e: [slot() for _ in range(3)] for e in (2,)}

    def far(e, o):
        each(two[e][o], "near_arrived" if o == 1 and e in far_by_z else "far")

    def far_done(e, o):
        if o == 1 and e in far_by_z:
            for (part, _), i in zip(shared[e], far_by_z[e]):
                arrived(i, part(2, 1, c))
        else:
            each(two[e][o], "far_arrived")
        if o == 0 and e in far_by_z:
            for (part, _), i in zip(shared[e], far_by_z[e]):
                push(i, part(2, 0, c), part(2, 0, c), z_peer)

    def gates(o):
        if o == 0:
            for load in loads:
                load.wait()
            numer[...] = jnp.zeros_like(numer)
        else:
            arrived(gate_slot, gate.at[1])
        side = jnp.where(zh == 1, o, 1 - o)
        g = gate[o].reshape(4 * experts, pooled.shape[1])
        for part in range(2):
            rows = pl.ds(part * half, half)
            logits = lax.dot_general(pooled[rows], g, (((1,), (1,)), ((), ())), preferred_element_type=F32)
            for e in range(experts):
                own = jnp.where(t == 0, logits[:, 4 * e : 4 * e + 2], logits[:, 4 * e + 2 : 4 * e + 4])
                weights[side, rows, 2 * e : 2 * e + 2] = jnp.exp(own)

    chunk = tokens // 3
    eo_slots = [slot() for _ in range(experts - 1)]
    last_slots = [slot() for _ in range(3)]
    assert used[0] <= send_sem.shape[0], used[0]

    def add_up(o, e, rows=slice(None)):
        values = eo[o, e, rows].astype(F32)
        for k in range(2):
            numer[k, rows] += weights[o, rows, 2 * e + k : 2 * e + k + 1] * values

    def layer_one(e, h, rows=slice(None)):
        for n in (2 * h, 2 * h + 1):
            cols = slice(256 * n, 256 * n + 256)
            w = w1[e, :, :, :, :, cols].reshape(16 * 208, 256)
            summed = jnp.dot(pooled[rows], w, preferred_element_type=F32)
            first[rows, cols] = jnp.maximum(summed, 0.0).astype(BF16)

    def layers_two_three(e, start=0, size=tokens):
        rows = pl.ds(start, size)
        for n in range(2):
            w = jnp.concatenate(
                [w23[e % 2, e // 2, :, :, :, q, n, 0:64].reshape(16 * 64, 128) for q in range(2)], axis=1
            )
            summed = jnp.dot(first[rows], w, preferred_element_type=F32)
            second[rows, 256 * n : 256 * n + 256] = jnp.maximum(summed, 0.0).astype(BF16)
        w = jnp.concatenate(
            [w23[e % 2, e // 2, :, :, :, :, n, 64:80].reshape(32 * 16, 128) for n in range(2)], axis=1
        )
        for part in range(2):
            rows = pl.ds(start + part * (size // 2), size // 2)
            summed = jnp.dot(second[rows], w, preferred_element_type=F32)
            eo[0, e, rows] = jnp.maximum(summed, 0.0).astype(BF16)

    def expert_done(e):
        layers_two_three(e)
        push(eo_slots[e], eo.at[0, e], eo.at[1, e], task_peer)
        add_up(0, e)

    def compute_last(e):
        for i in range(3):
            rows = pl.ds(i * chunk, chunk)
            for h in range(2):
                layer_one(e, h, rows)
            layers_two_three(e, i * chunk, chunk)
            push(last_slots[i], eo.at[0, e, rows], eo.at[1, e, rows], task_peer)
            add_up(0, e, rows)

    def finish(i):
        rows = pl.ds(i * chunk, chunk)
        arrived(last_slots[i], eo.at[1, experts - 1, rows])
        add_up(1, experts - 1, rows)
        for k in range(2):
            total = sum(weights[o, rows, 2 * e + k : 2 * e + k + 1] for o in range(2) for e in range(experts))
            mix = (numer[k, rows] / total).astype(BF16)
            tower = jnp.maximum(jnp.dot(mix, hidden_ref[k], preferred_element_type=F32), 0.0).astype(BF16)
            out_ref[k : k + 1, rows] = lax.dot_general(
                out_w_ref[k : k + 1, :], tower, (((1,), (1,)), ((), ())), preferred_element_type=F32
            )

    def others(e):
        arrived(eo_slots[e], eo.at[1, e])
        add_up(1, e)

    gates(0)
    first_round(0)
    quad(1)
    push(gate_slot, gate_hbm, gate.at[1], task_peer)
    first_round(1)
    quad(2)
    quad(3)
    first_done(0)
    near(0, 0)
    first_round(2)
    first_far(1)
    first_round(3)
    far(0, 0)
    gates(1)
    share(0, 0, (1, -1))
    first_done(1)
    share(0, 0, (0,))
    near(1, 0)
    first_far(2)
    first_far(3)
    z_done(0)
    far(1, 0)
    far_done(0, 0)
    share(1, 0, (0,))
    first_done(3)
    first_done(2)
    share(0, 1, (0,))
    near(2, 0)
    share(0, 0, (2,))
    z_done(1)
    far_done(1, 0)
    far(0, 1)
    share(1, 1, (0,))
    far(2, 0)
    share(0, 1, (1, -1))
    far(1, 1)
    share(1, 0, (2,))
    share(3, 0, (0,))
    near(3, 0)
    share(1, 1, (1, -1))
    far_done(0, 1)
    share(0, 1, (2,))
    z_done(2)
    share(1, 0, (1, -1))
    share(2, 0, (0,))
    far_done(2, 0)
    share(2, 0, (2,))
    share_arrived(0)
    share(2, 0, (1, -1))
    layer_one(0, 0)
    layer_one(0, 1)
    far_done(1, 1)
    z_done(3)
    share(1, 1, (2,))
    expert_done(0)
    far(3, 0)
    share(3, 0, (1, -1))
    share(2, 1, (0,))
    share(3, 1, (0,))
    share_arrived(1)
    layer_one(1, 0)
    layer_one(1, 1)
    far(2, 1)
    share(2, 1, (1, -1))
    far_done(2, 1)
    share(2, 1, (2,))
    expert_done(1)
    others(0)
    far(3, 1)
    share(3, 1, (1, -1))
    share_arrived(2)
    layer_one(2, 0)
    far_done(3, 0)
    layer_one(2, 1)
    share(3, 0, (2,))
    far_done(3, 1)
    share(3, 1, (2,))
    expert_done(2)
    others(1)
    share_arrived(3)
    compute_last(3)
    others(2)
    for i in range(3):
        finish(i)

    for copy in sent:
        copy.wait_send()


def per_device(pooled, gate_weight, w_first, w_second, w_third, tower_hidden, tower_out):
    tokens, width = pooled.shape
    experts = w_first.shape[0]
    any_, vmem = pl.BlockSpec(memory_space=pl.ANY), pl.BlockSpec(memory_space=pltpu.VMEM)
    slots = 300
    return pl.pallas_call(
        kernel,
        out_shape=jax.ShapeDtypeStruct((2, tokens), F32),
        in_specs=[any_] * 5 + [vmem, vmem],
        out_specs=vmem,
        scratch_shapes=[
            pltpu.VMEM((52, experts, 1024), BF16),
            pltpu.VMEM((experts, 16, 512), BF16),
            pltpu.VMEM((experts, 8, 256), BF16),
            pltpu.VMEM((QUAD, experts, BLOCK, 256), BF16),
            pltpu.VMEM((QUAD, experts, BLOCK, 256), BF16),
            pltpu.VMEM((experts, 4, 2, 2, 208, 1024), BF16),
            pltpu.VMEM((2, 2, 4, 2, 2, 2, 2, 80, 128), BF16),
            pltpu.VMEM((tokens, width), BF16),
            pltpu.VMEM((2, experts, 4, width), BF16),
            pltpu.VMEM((tokens, 1024), BF16),
            pltpu.VMEM((tokens, 512), BF16),
            pltpu.VMEM((2, experts, tokens, 256), BF16),
            pltpu.VMEM((2, tokens, 256), F32),
            pltpu.VMEM((2, tokens, 2 * experts), F32),
            pltpu.SemaphoreType.DMA((slots,)),
            pltpu.SemaphoreType.DMA((slots,)),
            pltpu.SemaphoreType.DMA((6,)),
        ],
        compiler_params=pltpu.CompilerParams(
            collective_id=0, has_side_effects=True, vmem_limit_bytes=67_000_000
        ),
    )(
        pooled, gate_weight.transpose(1, 2, 0), w_first.transpose(1, 0, 2), w_second, w_third, tower_hidden, tower_out
    ).T


def solution(mesh):
    torus = Mesh(mesh.devices.reshape(mesh.shape["task"], 4, 2, 4, 2), AXES)
    return jax.shard_map(
        per_device,
        mesh=torus,
        in_specs=(
            P(BATCH, None),
            P(None, "task", None),
            P("task", BATCH, None),
            P("task", BATCH, None),
            P("task", BATCH, None),
            P("task", None, None),
            P("task", None),
        ),
        out_specs=P(BATCH, "task"),
        check_vma=False,
    )
```

```python
import functools

import jax
import jax.numpy as jnp
from jax import lax
from jax.experimental import pallas as pl
from jax.experimental.pallas import tpu as pltpu
from jax.sharding import Mesh
from jax.sharding import PartitionSpec as P

AXES = ("task", "batch_0", "batch_1", "batch_2", "batch_3")
BATCH = AXES[1:]
MESH = pl.DeviceIdType.MESH
BF16 = jnp.bfloat16
F32 = jnp.float32

W1_ROWS, W2_ROWS, W3_ROWS = 52, 8, 4
QUAD = 4
BLOCK = W1_ROWS + W2_ROWS + W3_ROWS


def one_hot(rows, source):
    row = lax.broadcasted_iota(jnp.int32, (rows, QUAD * BLOCK), 0)
    column = lax.broadcasted_iota(jnp.int32, (rows, QUAD * BLOCK), 1)
    return jnp.where(source(row) == column, 1.0, 0.0).astype(BF16)


def picked(selector, values):
    return jnp.dot(selector, values, preferred_element_type=F32).astype(BF16)


def kernel(
    pooled_hbm, gate_hbm, first_hbm, second_hbm, third_hbm, hidden_ref, out_w_ref, out_ref,
    raw1, raw2, raw3, block, staged, w1, w23, pooled, gate, first, second, eo, numer, weights, send_sem, recv_sem, local_sem,
):
    t, y, zh, x, c = (lax.axis_index(a) for a in AXES)
    xp, xq = x // 2, lax.rem(x, 2)
    j = 2 * xq + c
    tq = jnp.where(zh == 1, t, 1 - t)
    experts = w1.shape[0]
    tokens = pooled.shape[0]

    def at(pos, k):
        return lax.rem(pos + (k + 4), 4)

    core_peer = (t, y, zh, x, 1 - c)
    z_peer = (1 - t, y, 1 - zh, x, c)
    task_peer = (1 - t, y, zh, x, c)
    x_dev = lambda k: (t, y, zh, at(x, k), c)
    y_dev = lambda k: (t, at(y, k), zh, x, c)

    def quad_dev(d):
        dx, dc = d // 2, d % 2
        return (tq, y, zh, 2 * xp + (1 - xq if dx else xq), 1 - c if dc else c)

    used = [0]
    sent = []

    def slot():
        used[0] += 1
        return used[0] - 1

    def push(i, src, dst, device):
        copy = pltpu.make_async_remote_copy(
            src_ref=src, dst_ref=dst, send_sem=send_sem.at[i], recv_sem=recv_sem.at[i],
            device_id=device, device_id_type=MESH,
        )
        copy.start()
        sent.append(copy)

    def arrived(i, dst):
        pltpu.make_async_remote_copy(
            src_ref=dst, dst_ref=dst, send_sem=send_sem.at[i], recv_sem=recv_sem.at[i],
            device_id=core_peer, device_id_type=MESH,
        ).wait_recv()

    half = tokens // 2
    shards = [
        pltpu.make_async_copy(src, dst, local_sem.at[i])
        for i, (src, dst) in enumerate([(first_hbm, raw1), (second_hbm, raw2), (third_hbm, raw3)])
    ]
    loads = [
        pltpu.make_async_copy(pooled_hbm.at[pl.ds(k * half, half)], pooled.at[pl.ds(k * half, half)], local_sem.at[3 + k])
        for k in range(2)
    ]
    loads.append(pltpu.make_async_copy(gate_hbm, gate.at[0], local_sem.at[5]))
    for load in shards + loads:
        load.start()

    barrier = pltpu.get_barrier_semaphore()
    peers = [x_dev(1), x_dev(-1), x_dev(2), y_dev(1), y_dev(-1), y_dev(2), z_peer, core_peer, task_peer] + [quad_dev(d) for d in range(1, QUAD)]
    for device in peers:
        pl.semaphore_signal(barrier, inc=1, device_id=device, device_id_type=MESH)

    for load in shards:
        load.wait()

    def place(rows, columns, source):
        row = lax.broadcasted_iota(jnp.int32, (rows, columns), 0)
        column = lax.broadcasted_iota(jnp.int32, (rows, columns), 1)
        return jnp.where(source(row) == column, 1.0, 0.0).astype(BF16)

    def band(row, start, size, source):
        return jnp.where((row >= start) & (row < start + size), source, -1)

    def build(e):
        put1 = place(BLOCK, experts * W1_ROWS, lambda r: band(r, 0, W1_ROWS, experts * r + e))
        rows1 = jnp.dot(put1, raw1[...].reshape(experts * W1_ROWS, 1024), preferred_element_type=F32)
        rows2, rows3 = [], []
        for side in range(2):
            put2 = place(BLOCK, 16, lambda r: band(r, W1_ROWS, W2_ROWS, r - W1_ROWS + W2_ROWS * side))
            put3 = place(BLOCK, 8, lambda r: band(r, W1_ROWS + W2_ROWS, W3_ROWS, r - W1_ROWS - W2_ROWS + W3_ROWS * side))
            rows2.append(jnp.dot(put2, raw2[e], preferred_element_type=F32))
            rows3.append(jnp.dot(put3, raw3[e], preferred_element_type=F32))
        for member in range(QUAD):
            q, n = member // 2, member % 2
            for side in range(2):
                col1, col2, col3 = 512 * n + 256 * side + 128 * q, 256 * n + 128 * q, 128 * n
                both = rows1[:, col1 : col1 + 128] + rows2[side][:, col2 : col2 + 128] + rows3[side][:, col3 : col3 + 128]
                block[member, e, :, 128 * side : 128 * side + 128] = both.astype(BF16)

    build(0)
    pl.semaphore_wait(barrier, len(peers))

    def member(d):
        return 2 * ((1 - xq) if d // 2 else xq) + ((1 - c) if d % 2 else c)

    quad_slots = [[slot() for _ in range(QUAD)] for _ in range(experts)]
    own_far = [
        pltpu.make_async_remote_copy(
            src_ref=block.at[j, e], dst_ref=staged.at[j, e], send_sem=send_sem.at[quad_slots[e][0]],
            recv_sem=recv_sem.at[quad_slots[e][0]], device_id=task_peer, device_id_type=MESH,
        )
        for e in range(experts)
    ]

    def quad(e):
        for d in range(1, QUAD):
            push(quad_slots[e][d], block.at[member(d), e], staged.at[j, e], quad_dev(d))

        @pl.when(zh == 0)
        def _():
            own_far[e].start()

        @pl.when(zh == 1)
        def _():
            staged[j, e] = block[j, e]

    quad(0)
    for e in range(1, experts):
        build(e)
    gate_slot = slot()

    def w1_source(r):
        return r + (BLOCK - W1_ROWS) * (
            (r >= W1_ROWS).astype(jnp.int32) + (r >= 2 * W1_ROWS).astype(jnp.int32) + (r >= 3 * W1_ROWS).astype(jnp.int32)
        )

    def half_source(r, unit, side, base):
        member, within = r // (2 * unit), lax.rem(r, 2 * unit)
        return jnp.where(within // unit == side, BLOCK * member + base + lax.rem(within, unit), -1)

    pick1 = one_hot(QUAD * W1_ROWS, w1_source)
    pick2 = [one_hot(QUAD * 16, lambda r, s=s: half_source(r, W2_ROWS, s, W1_ROWS)) for s in range(2)]
    pick3 = [
        one_hot(16, lambda r, s=s: jnp.where(
            half_source(r, W3_ROWS, s, W1_ROWS + W2_ROWS) >= 0,
            half_source(r, W3_ROWS, s, W1_ROWS + W2_ROWS) + 2 * BLOCK * xq, -1))
        for s in range(2)
    ]
    col0 = pl.multiple_of(512 * c, 128)

    def w1_cols(h, xq_):
        return pl.ds(pl.multiple_of(512 * c + 256 * h + 128 * xq_, 128), 128)

    def pack(e):
        for d in range(1, QUAD):
            arrived(quad_slots[e][d], staged.at[member(d), e])

        @pl.when(zh == 0)
        def _():
            own_far[e].wait()

        rows = staged[:, e].reshape(QUAD * BLOCK, 256)
        w1_part = picked(pick1, rows)
        w1[e, y, zh, xp, :, w1_cols(0, xq)] = w1_part[:, :128]
        w1[e, y, zh, xp, :, w1_cols(1, xq)] = w1_part[:, 128:]
        w23[e % 2, e // 2, y, zh, xp, xq, c, 0:64] = picked(
            jnp.concatenate(pick2, axis=1), jnp.concatenate([rows[:, :128], rows[:, 128:]], axis=0)
        )
        w23[e % 2, e // 2, y, zh, xp, xq, c, 64:80] = picked(
            jnp.concatenate(pick3, axis=1), jnp.concatenate([rows[:, :128], rows[:, 128:]], axis=0)
        )

    def plane(o):
        return zh if o == 0 else 1 - zh

    def a1(e, k):
        x_ = at(x, k)
        return w1.at[e, y, zh, x_ // 2, :, w1_cols(0, lax.rem(x_, 2))]

    def b1(e, k):
        return w1.at[e, at(y, k), zh, xp, :, w1_cols(1, xq)]

    def c1(e, k):
        if e % 2 == 0:
            x_ = at(x, k)
            return w23.at[0, e // 2, y, zh, x_ // 2, lax.rem(x_, 2), c]
        return w23.at[1, e // 2, at(y, k), zh, xp, xq, c]

    def a2(e, k, o, core, rows=slice(None)):
        return w1.at[e, at(y, k), plane(o), rows, :, pl.ds(pl.multiple_of(512 * core, 128), 256)]

    def b2(e, k, o, core, rows=slice(None)):
        x_ = at(x, k)
        cols = pl.ds(pl.multiple_of(512 * core + 256 + 128 * lax.rem(x_, 2), 128), 128)
        return w1.at[e, rows, plane(o), x_ // 2, :, cols]

    def c2(e, k, o, core, rows=slice(None)):
        if e % 2 == 0:
            return w23.at[0, e // 2, at(y, k), plane(o), rows, :, core]
        x_ = at(x, k)
        return w23.at[1, e // 2, rows, plane(o), x_ // 2, lax.rem(x_, 2), core]

    class Ring:
        def __init__(self, device, part, ways, direct=False):
            self.device, self.part, self.ways, self.direct = device, part, ways, direct
            self.slots = {k: slot() for k in (1, -1)}
            self.far_slots = {k: slot() for k in ways}

        def near(self):
            for k in (1, -1):
                push(self.slots[k], self.part(0), self.part(0), self.device(k))
            if self.direct:
                for k in self.ways:
                    push(self.far_slots[k], self.part(0), self.part(0), self.device(2))

        def near_arrived(self):
            for k in (1, -1):
                arrived(self.slots[k], self.part(-k))

        def far(self):
            self.near_arrived()
            for k, half in self.ways.items():
                push(self.far_slots[k], half(-k), half(-k), self.device(k))

        def far_arrived(self):
            for k, half in self.ways.items():
                arrived(self.far_slots[k], half(2))

    one, two, z_slots, shared = [], [], [], []
    for e in range(experts):
        x_first, y_first = (x_dev, y_dev), (y_dev, x_dev)
        parts = [
            (x_first, lambda k, e=e: a1(e, k), functools.partial(a2, e), 2),
            (y_first, lambda k, e=e: b1(e, k), functools.partial(b2, e), 4),
            (x_first if e % 2 == 0 else y_first, lambda k, e=e: c1(e, k), functools.partial(c2, e), 2 if e % 2 == 0 else 4),
        ]
        one.append([Ring(d[0], p1, {(1 if (e + i) % 2 == 0 else -1): p1}, e < 1) for i, (d, p1, _, _) in enumerate(parts)])
        two.append([
            [
                Ring(d[1], lambda k, p2=p2, o=o: p2(k, o, c), {
                    1: lambda k, p2=p2, o=o, n=n: p2(k, o, c, pl.ds(0, n // 2)),
                    -1: lambda k, p2=p2, o=o, n=n: p2(k, o, c, pl.ds(n // 2, n // 2)),
                })
                for d, _, p2, n in parts
            ]
            for o in range(2)
        ])
        z_slots.append([slot() for _ in parts])
        shared.append([(p2, {(k, o): slot() for k in (0, 1, -1, 2) for o in range(2)}) for _, _, p2, _ in parts])

    def share(e, o, which):
        for part, slots in shared[e]:
            for k in which:
                push(slots[k, o], part(k, o, c), part(k, o, c), core_peer)

    def share_arrived(e):
        for part, slots in shared[e]:
            for (k, o), i in slots.items():
                arrived(i, part(k, o, 1 - c))

    def each(rings, step):
        for ring in rings:
            getattr(ring, step)()

    def first_round(e):
        pack(e)
        each(one[e], "near")

    def first_far(e):
        each(one[e], "far")

    def first_done(e):
        if e < 1:
            each(one[e], "near_arrived")
        each(one[e], "far_arrived")
        for (part, _), i in zip(shared[e], z_slots[e]):
            push(i, part(0, 0, c), part(0, 0, c), z_peer)

    def near(e, o):
        each(two[e][o], "near")

    def z_done(e):
        for (part, _), i in zip(shared[e], z_slots[e]):
            arrived(i, part(0, 1, c))
        near(e, 1)

    far_by_z = {e: [slot() for _ in range(3)] for e in (2,)}

    def far(e, o):
        each(two[e][o], "near_arrived" if o == 1 and e in far_by_z else "far")

    def far_done(e, o):
        if o == 1 and e in far_by_z:
            for (part, _), i in zip(shared[e], far_by_z[e]):
                arrived(i, part(2, 1, c))
        else:
            each(two[e][o], "far_arrived")
        if o == 0 and e in far_by_z:
            for (part, _), i in zip(shared[e], far_by_z[e]):
                push(i, part(2, 0, c), part(2, 0, c), z_peer)

    def gates(o):
        if o == 0:
            for load in loads:
                load.wait()
            numer[...] = jnp.zeros_like(numer)
        else:
            arrived(gate_slot, gate.at[1])
        side = jnp.where(zh == 1, o, 1 - o)
        g = gate[o].reshape(4 * experts, pooled.shape[1])
        for part in range(2):
            rows = pl.ds(part * half, half)
            logits = lax.dot_general(pooled[rows], g, (((1,), (1,)), ((), ())), preferred_element_type=F32)
            for e in range(experts):
                own = jnp.where(t == 0, logits[:, 4 * e : 4 * e + 2], logits[:, 4 * e + 2 : 4 * e + 4])
                weights[side, rows, 2 * e : 2 * e + 2] = jnp.exp(own)

    chunk = tokens // 3
    eo_slots = [[slot() for _ in range(3)] for _ in range(experts)]
    assert used[0] <= send_sem.shape[0], used[0]

    def add_up(o, e, rows=slice(None)):
        values = eo[o, e, rows].astype(F32)
        for k in range(2):
            numer[k, rows] += weights[o, rows, 2 * e + k : 2 * e + k + 1] * values

    def layer_one(e, h, rows=slice(None)):
        for n in (2 * h, 2 * h + 1):
            cols = slice(256 * n, 256 * n + 256)
            w = w1[e, :, :, :, :, cols].reshape(16 * 208, 256)
            summed = jnp.dot(pooled[rows], w, preferred_element_type=F32)
            first[rows, cols] = jnp.maximum(summed, 0.0).astype(BF16)

    def layers_two_three(e, start=0, size=tokens):
        rows = pl.ds(start, size)
        for n in range(2):
            w = jnp.concatenate(
                [w23[e % 2, e // 2, :, :, :, q, n, 0:64].reshape(16 * 64, 128) for q in range(2)], axis=1
            )
            summed = jnp.dot(first[rows], w, preferred_element_type=F32)
            second[rows, 256 * n : 256 * n + 256] = jnp.maximum(summed, 0.0).astype(BF16)
        w = jnp.concatenate(
            [w23[e % 2, e // 2, :, :, :, :, n, 64:80].reshape(32 * 16, 128) for n in range(2)], axis=1
        )
        for part in range(2):
            rows = pl.ds(start + part * (size // 2), size // 2)
            summed = jnp.dot(second[rows], w, preferred_element_type=F32)
            eo[0, e, rows] = jnp.maximum(summed, 0.0).astype(BF16)

    def compute(e, i):
        rows = pl.ds(i * chunk, chunk)
        for h in range(2):
            layer_one(e, h, rows)
        layers_two_three(e, i * chunk, chunk)
        push(eo_slots[e][i], eo.at[0, e, rows], eo.at[1, e, rows], task_peer)
        add_up(0, e, rows)

    def others(e):
        for i in range(3):
            arrived(eo_slots[e][i], eo.at[1, e, pl.ds(i * chunk, chunk)])
        add_up(1, e)

    def finish(i):
        rows = pl.ds(i * chunk, chunk)
        arrived(eo_slots[experts - 1][i], eo.at[1, experts - 1, rows])
        add_up(1, experts - 1, rows)
        for k in range(2):
            total = sum(weights[o, rows, 2 * e + k : 2 * e + k + 1] for o in range(2) for e in range(experts))
            mix = (numer[k, rows] / total).astype(BF16)
            tower = jnp.maximum(jnp.dot(mix, hidden_ref[k], preferred_element_type=F32), 0.0).astype(BF16)
            out_ref[k : k + 1, rows] = lax.dot_general(
                out_w_ref[k : k + 1, :], tower, (((1,), (1,)), ((), ())), preferred_element_type=F32
            )

    gates(0)
    quad(1)
    first_round(0)
    quad(2)
    first_round(1)
    quad(3)
    first_round(2)
    first_round(3)
    first_done(0)
    first_far(1)
    near(0, 0)
    first_far(2)
    first_far(3)
    first_done(1)
    near(1, 0)
    first_done(2)
    z_done(0)
    push(gate_slot, gate_hbm, gate.at[1], task_peer)
    near(2, 0)
    far(0, 1)
    far(1, 0)
    share(1, 0, (1, -1))
    z_done(1)
    far(0, 0)
    far(2, 0)
    first_done(3)
    share(0, 0, (1, -1))
    far_done(0, 1)
    share(0, 1, (0,))
    share(2, 0, (0,))
    far_done(1, 0)
    far(1, 1)
    z_done(2)
    share(0, 1, (1, -1))
    share(2, 1, (0,))
    share(0, 0, (0,))
    far_done(0, 0)
    share(0, 0, (2,))
    near(3, 0)
    share(0, 1, (2,))
    gates(1)
    share(2, 0, (1, -1))
    share(1, 1, (0,))
    share_arrived(0)
    share(1, 0, (2,))
    z_done(3)
    far_done(2, 0)
    share(2, 0, (2,))
    share(1, 1, (1, -1))
    share(3, 1, (0,))
    share(1, 0, (0,))
    compute(0, 0)
    share(3, 0, (0,))
    far_done(1, 1)
    share(1, 1, (2,))
    compute(0, 1)
    compute(0, 2)
    far(2, 1)
    share_arrived(1)
    compute(1, 0)
    compute(1, 1)
    far_done(2, 1)
    share(2, 1, (1, -1))
    far(3, 0)
    share(2, 1, (2,))
    compute(1, 2)
    others(0)
    far(3, 1)
    share_arrived(2)
    share(3, 1, (1, -1))
    compute(2, 0)
    share(3, 0, (1, -1))
    far_done(3, 0)
    share(3, 0, (2,))
    compute(2, 1)
    far_done(3, 1)
    share(3, 1, (2,))
    compute(2, 2)
    share_arrived(3)
    compute(3, 0)
    compute(3, 1)
    others(1)
    others(2)
    compute(3, 2)
    for i in range(3):
        finish(i)

    for copy in sent:
        copy.wait_send()


def per_device(pooled, gate_weight, w_first, w_second, w_third, tower_hidden, tower_out):
    tokens, width = pooled.shape
    experts = w_first.shape[0]
    any_, vmem = pl.BlockSpec(memory_space=pl.ANY), pl.BlockSpec(memory_space=pltpu.VMEM)
    slots = 300
    return pl.pallas_call(
        kernel,
        out_shape=jax.ShapeDtypeStruct((2, tokens), F32),
        in_specs=[any_] * 5 + [vmem, vmem],
        out_specs=vmem,
        scratch_shapes=[
            pltpu.VMEM((52, experts, 1024), BF16),
            pltpu.VMEM((experts, 16, 512), BF16),
            pltpu.VMEM((experts, 8, 256), BF16),
            pltpu.VMEM((QUAD, experts, BLOCK, 256), BF16),
            pltpu.VMEM((QUAD, experts, BLOCK, 256), BF16),
            pltpu.VMEM((experts, 4, 2, 2, 208, 1024), BF16),
            pltpu.VMEM((2, 2, 4, 2, 2, 2, 2, 80, 128), BF16),
            pltpu.VMEM((tokens, width), BF16),
            pltpu.VMEM((2, experts, 4, width), BF16),
            pltpu.VMEM((tokens, 1024), BF16),
            pltpu.VMEM((tokens, 512), BF16),
            pltpu.VMEM((2, experts, tokens, 256), BF16),
            pltpu.VMEM((2, tokens, 256), F32),
            pltpu.VMEM((2, tokens, 2 * experts), F32),
            pltpu.SemaphoreType.DMA((slots,)),
            pltpu.SemaphoreType.DMA((slots,)),
            pltpu.SemaphoreType.DMA((6,)),
        ],
        compiler_params=pltpu.CompilerParams(
            collective_id=0, has_side_effects=True, vmem_limit_bytes=67_000_000
        ),
    )(
        pooled, gate_weight.transpose(1, 2, 0), w_first.transpose(1, 0, 2), w_second, w_third, tower_hidden, tower_out
    ).T


def solution(mesh):
    torus = Mesh(mesh.devices.reshape(mesh.shape["task"], 4, 2, 4, 2), AXES)
    return jax.shard_map(
        per_device,
        mesh=torus,
        in_specs=(
            P(BATCH, None),
            P(None, "task", None),
            P("task", BATCH, None),
            P("task", BATCH, None),
            P("task", BATCH, None),
            P("task", None, None),
            P("task", None),
        ),
        out_specs=P(BATCH, "task"),
        check_vma=False,
    )
```

```python
import functools

import jax
import jax.numpy as jnp
from jax import lax
from jax.experimental import pallas as pl
from jax.experimental.pallas import tpu as pltpu
from jax.sharding import Mesh
from jax.sharding import PartitionSpec as P

AXES = ("task", "batch_0", "batch_1", "batch_2", "batch_3")
BATCH = AXES[1:]
MESH = pl.DeviceIdType.MESH
BF16 = jnp.bfloat16
F32 = jnp.float32

W1_ROWS, W2_ROWS, W3_ROWS = 52, 8, 4
QUAD = 4
BLOCK = W1_ROWS + W2_ROWS + W3_ROWS


def one_hot(rows, source):
    row = lax.broadcasted_iota(jnp.int32, (rows, QUAD * BLOCK), 0)
    column = lax.broadcasted_iota(jnp.int32, (rows, QUAD * BLOCK), 1)
    return jnp.where(source(row) == column, 1.0, 0.0).astype(BF16)


def picked(selector, values):
    return jnp.dot(selector, values, preferred_element_type=F32).astype(BF16)


def kernel(
    pooled_hbm, gate_hbm, first_hbm, second_hbm, third_hbm, hidden_ref, out_w_ref, out_ref,
    raw1, raw2, raw3, block, staged, w1, w23, pooled, gate, first, second, partial, eo, numer, weights, send_sem, recv_sem, local_sem,
):
    t, y, zh, x, c = (lax.axis_index(a) for a in AXES)
    xp, xq = x // 2, lax.rem(x, 2)
    j = 2 * xq + c
    tq = jnp.where(zh == 1, t, 1 - t)
    experts = w1.shape[0]
    tokens = pooled.shape[0]

    def at(pos, k):
        return lax.rem(pos + (k + 4), 4)

    core_peer = (t, y, zh, x, 1 - c)
    z_peer = (1 - t, y, 1 - zh, x, c)
    task_peer = (1 - t, y, zh, x, c)
    x_dev = lambda k: (t, y, zh, at(x, k), c)
    y_dev = lambda k: (t, at(y, k), zh, x, c)

    def quad_dev(d):
        dx, dc = d // 2, d % 2
        return (tq, y, zh, 2 * xp + (1 - xq if dx else xq), 1 - c if dc else c)

    used = [0]
    sent = []

    def slot():
        used[0] += 1
        return used[0] - 1

    def push(i, src, dst, device):
        copy = pltpu.make_async_remote_copy(
            src_ref=src, dst_ref=dst, send_sem=send_sem.at[i], recv_sem=recv_sem.at[i],
            device_id=device, device_id_type=MESH,
        )
        copy.start()
        sent.append(copy)

    def arrived(i, dst):
        pltpu.make_async_remote_copy(
            src_ref=dst, dst_ref=dst, send_sem=send_sem.at[i], recv_sem=recv_sem.at[i],
            device_id=core_peer, device_id_type=MESH,
        ).wait_recv()

    half = tokens // 2
    shards = [
        pltpu.make_async_copy(src, dst, local_sem.at[i])
        for i, (src, dst) in enumerate([(first_hbm, raw1), (second_hbm, raw2), (third_hbm, raw3)])
    ]
    loads = [
        pltpu.make_async_copy(pooled_hbm.at[pl.ds(k * half, half)], pooled.at[pl.ds(k * half, half)], local_sem.at[3 + k])
        for k in range(2)
    ]
    loads.append(pltpu.make_async_copy(gate_hbm, gate.at[0], local_sem.at[5]))
    for load in shards + loads:
        load.start()

    barrier = pltpu.get_barrier_semaphore()
    peers = [x_dev(1), x_dev(-1), x_dev(2), y_dev(1), y_dev(-1), y_dev(2), z_peer, core_peer, task_peer] + [quad_dev(d) for d in range(1, QUAD)]
    for device in peers:
        pl.semaphore_signal(barrier, inc=1, device_id=device, device_id_type=MESH)

    for load in shards:
        load.wait()

    def place(rows, columns, source):
        row = lax.broadcasted_iota(jnp.int32, (rows, columns), 0)
        column = lax.broadcasted_iota(jnp.int32, (rows, columns), 1)
        return jnp.where(source(row) == column, 1.0, 0.0).astype(BF16)

    def band(row, start, size, source):
        return jnp.where((row >= start) & (row < start + size), source, -1)

    def build(e):
        put1 = place(BLOCK, experts * W1_ROWS, lambda r: band(r, 0, W1_ROWS, experts * r + e))
        rows1 = jnp.dot(put1, raw1[...].reshape(experts * W1_ROWS, 1024), preferred_element_type=F32)
        rows2, rows3 = [], []
        for side in range(2):
            put2 = place(BLOCK, 16, lambda r: band(r, W1_ROWS, W2_ROWS, r - W1_ROWS + W2_ROWS * side))
            put3 = place(BLOCK, 8, lambda r: band(r, W1_ROWS + W2_ROWS, W3_ROWS, r - W1_ROWS - W2_ROWS + W3_ROWS * side))
            rows2.append(jnp.dot(put2, raw2[e], preferred_element_type=F32))
            rows3.append(jnp.dot(put3, raw3[e], preferred_element_type=F32))
        for member in range(QUAD):
            q, n = member // 2, member % 2
            for side in range(2):
                col1, col2, col3 = 512 * n + 256 * side + 128 * q, 256 * n + 128 * q, 128 * n
                both = rows1[:, col1 : col1 + 128] + rows2[side][:, col2 : col2 + 128] + rows3[side][:, col3 : col3 + 128]
                block[member, e, :, 128 * side : 128 * side + 128] = both.astype(BF16)

    build(0)
    pl.semaphore_wait(barrier, len(peers))

    def member(d):
        return 2 * ((1 - xq) if d // 2 else xq) + ((1 - c) if d % 2 else c)

    quad_slots = [[slot() for _ in range(QUAD)] for _ in range(experts)]
    own_far = [
        pltpu.make_async_remote_copy(
            src_ref=block.at[j, e], dst_ref=staged.at[j, e], send_sem=send_sem.at[quad_slots[e][0]],
            recv_sem=recv_sem.at[quad_slots[e][0]], device_id=task_peer, device_id_type=MESH,
        )
        for e in range(experts)
    ]

    def quad(e):
        for d in range(1, QUAD):
            push(quad_slots[e][d], block.at[member(d), e], staged.at[j, e], quad_dev(d))

        @pl.when(zh == 0)
        def _():
            own_far[e].start()

        @pl.when(zh == 1)
        def _():
            staged[j, e] = block[j, e]

    quad(0)
    for e in range(1, experts):
        build(e)
    gate_slot = slot()

    def w1_source(r):
        return r + (BLOCK - W1_ROWS) * (
            (r >= W1_ROWS).astype(jnp.int32) + (r >= 2 * W1_ROWS).astype(jnp.int32) + (r >= 3 * W1_ROWS).astype(jnp.int32)
        )

    def half_source(r, unit, side, base):
        member, within = r // (2 * unit), lax.rem(r, 2 * unit)
        return jnp.where(within // unit == side, BLOCK * member + base + lax.rem(within, unit), -1)

    pick1 = one_hot(QUAD * W1_ROWS, w1_source)
    pick2 = [one_hot(QUAD * 16, lambda r, s=s: half_source(r, W2_ROWS, s, W1_ROWS)) for s in range(2)]
    pick3 = [
        one_hot(16, lambda r, s=s: jnp.where(
            half_source(r, W3_ROWS, s, W1_ROWS + W2_ROWS) >= 0,
            half_source(r, W3_ROWS, s, W1_ROWS + W2_ROWS) + 2 * BLOCK * xq, -1))
        for s in range(2)
    ]
    col0 = pl.multiple_of(512 * c, 128)

    def w1_cols(h, xq_):
        return pl.ds(pl.multiple_of(512 * c + 256 * h + 128 * xq_, 128), 128)

    def pack(e):
        for d in range(1, QUAD):
            arrived(quad_slots[e][d], staged.at[member(d), e])

        @pl.when(zh == 0)
        def _():
            own_far[e].wait()

        rows = staged[:, e].reshape(QUAD * BLOCK, 256)
        w1_part = picked(pick1, rows)
        w1[e, y, zh, xp, :, w1_cols(0, xq)] = w1_part[:, :128]
        w1[e, y, zh, xp, :, w1_cols(1, xq)] = w1_part[:, 128:]
        w23[e % 2, e // 2, y, zh, xp, xq, c, 0:64] = picked(
            jnp.concatenate(pick2, axis=1), jnp.concatenate([rows[:, :128], rows[:, 128:]], axis=0)
        )
        w23[e % 2, e // 2, y, zh, xp, xq, c, 64:80] = picked(
            jnp.concatenate(pick3, axis=1), jnp.concatenate([rows[:, :128], rows[:, 128:]], axis=0)
        )

    def plane(o):
        return zh if o == 0 else 1 - zh

    def a1(e, k):
        x_ = at(x, k)
        return w1.at[e, y, zh, x_ // 2, :, w1_cols(0, lax.rem(x_, 2))]

    def b1(e, k):
        return w1.at[e, at(y, k), zh, xp, :, w1_cols(1, xq)]

    def c1(e, k):
        if e % 2 == 0:
            x_ = at(x, k)
            return w23.at[0, e // 2, y, zh, x_ // 2, lax.rem(x_, 2), c]
        return w23.at[1, e // 2, at(y, k), zh, xp, xq, c]

    def a2(e, k, o, core, rows=slice(None)):
        return w1.at[e, at(y, k), plane(o), rows, :, pl.ds(pl.multiple_of(512 * core, 128), 256)]

    def b2(e, k, o, core, rows=slice(None)):
        x_ = at(x, k)
        cols = pl.ds(pl.multiple_of(512 * core + 256 + 128 * lax.rem(x_, 2), 128), 128)
        return w1.at[e, rows, plane(o), x_ // 2, :, cols]

    def c2(e, k, o, core, rows=slice(None)):
        if e % 2 == 0:
            return w23.at[0, e // 2, at(y, k), plane(o), rows, :, core]
        x_ = at(x, k)
        return w23.at[1, e // 2, rows, plane(o), x_ // 2, lax.rem(x_, 2), core]

    class Ring:
        def __init__(self, device, part, ways, direct=False):
            self.device, self.part, self.ways, self.direct = device, part, ways, direct
            self.slots = {k: slot() for k in (1, -1)}
            self.far_slots = {k: slot() for k in ways}

        def near(self):
            for k in (1, -1):
                push(self.slots[k], self.part(0), self.part(0), self.device(k))
            if self.direct:
                for k in self.ways:
                    push(self.far_slots[k], self.part(0), self.part(0), self.device(2))

        def near_arrived(self):
            for k in (1, -1):
                arrived(self.slots[k], self.part(-k))

        def far(self):
            self.near_arrived()
            for k, half in self.ways.items():
                push(self.far_slots[k], half(-k), half(-k), self.device(k))

        def far_arrived(self):
            for k, half in self.ways.items():
                arrived(self.far_slots[k], half(2))

    one, two, z_slots, shared = [], [], [], []
    for e in range(experts):
        x_first, y_first = (x_dev, y_dev), (y_dev, x_dev)
        parts = [
            (x_first, lambda k, e=e: a1(e, k), functools.partial(a2, e), 2),
            (y_first, lambda k, e=e: b1(e, k), functools.partial(b2, e), 4),
            (x_first if e % 2 == 0 else y_first, lambda k, e=e: c1(e, k), functools.partial(c2, e), 2 if e % 2 == 0 else 4),
        ]
        one.append([Ring(d[0], p1, {(1 if (e + i) % 2 == 0 else -1): p1}, e < 2) for i, (d, p1, _, _) in enumerate(parts)])
        two.append([
            [
                Ring(d[1], lambda k, p2=p2, o=o: p2(k, o, c), {
                    1: lambda k, p2=p2, o=o, n=n: p2(k, o, c, pl.ds(0, n // 2)),
                    -1: lambda k, p2=p2, o=o, n=n: p2(k, o, c, pl.ds(n // 2, n // 2)),
                })
                for d, _, p2, n in parts
            ]
            for o in range(2)
        ])
        z_slots.append([slot() for _ in parts])
        shared.append([(p2, {(k, o): slot() for k in (0, 1, -1, 2) for o in range(2)}) for _, _, p2, _ in parts])

    def share(e, o, which):
        for part, slots in shared[e]:
            for k in which:
                push(slots[k, o], part(k, o, c), part(k, o, c), core_peer)

    def share_arrived(e, o):
        for part, slots in shared[e]:
            for k in (0, 1, -1, 2):
                arrived(slots[k, o], part(k, o, 1 - c))

    def each(rings, step):
        for ring in rings:
            getattr(ring, step)()

    def first_round(e):
        pack(e)
        each(one[e], "near")

    def first_far(e):
        each(one[e], "far")

    def first_done(e):
        if e < 2:
            each(one[e], "near_arrived")
        each(one[e], "far_arrived")
        for (part, _), i in zip(shared[e], z_slots[e]):
            push(i, part(0, 0, c), part(0, 0, c), z_peer)

    def near(e, o):
        each(two[e][o], "near")

    def z_done(e):
        for (part, _), i in zip(shared[e], z_slots[e]):
            arrived(i, part(0, 1, c))
        near(e, 1)

    far_by_z = {e: [slot() for _ in range(3)] for e in (2,)}

    def far(e, o):
        each(two[e][o], "near_arrived" if o == 1 and e in far_by_z else "far")

    def far_done(e, o):
        if o == 1 and e in far_by_z:
            for (part, _), i in zip(shared[e], far_by_z[e]):
                arrived(i, part(2, 1, c))
        else:
            each(two[e][o], "far_arrived")
        if o == 0 and e in far_by_z:
            for (part, _), i in zip(shared[e], far_by_z[e]):
                push(i, part(2, 0, c), part(2, 0, c), z_peer)

    def gates(o):
        if o == 0:
            for load in loads:
                load.wait()
            numer[...] = jnp.zeros_like(numer)
        else:
            arrived(gate_slot, gate.at[1])
        side = jnp.where(zh == 1, o, 1 - o)
        g = gate[o].reshape(4 * experts, pooled.shape[1])
        for part in range(2):
            rows = pl.ds(part * half, half)
            logits = lax.dot_general(pooled[rows], g, (((1,), (1,)), ((), ())), preferred_element_type=F32)
            for e in range(experts):
                own = jnp.where(t == 0, logits[:, 4 * e : 4 * e + 2], logits[:, 4 * e + 2 : 4 * e + 4])
                weights[side, rows, 2 * e : 2 * e + 2] = jnp.exp(own)

    chunk = tokens // 3
    eo_slots = [[slot() for _ in range(3)] for _ in range(experts)]
    assert used[0] <= send_sem.shape[0], used[0]

    def add_up(o, e, rows=slice(None)):
        values = eo[o, e, rows].astype(F32)
        for k in range(2):
            numer[k, rows] += weights[o, rows, 2 * e + k : 2 * e + k + 1] * values

    def by_plane():
        run, rows_each = 2 * 208, tokens // 12

        @pl.loop(0, 12)
        def _(i):
            rows = pl.ds(pl.multiple_of(i * rows_each, rows_each), rows_each)
            values = pooled[rows]
            pooled[rows] = jnp.concatenate(
                [values[:, (2 * n + p) * run : (2 * n + p + 1) * run] for p in range(2) for n in range(4)], axis=1
            )

    def plane_sum(e, o, n, rows):
        p = plane(o)
        depth = 8 * 208
        w = w1[e, :, p, :, :, 256 * n : 256 * n + 256].reshape(depth, 256)
        return jnp.dot(pooled[rows, pl.ds(pl.multiple_of(p * depth, 128), depth)], w, preferred_element_type=F32)

    def early(e, h):
        for n in (2 * h, 2 * h + 1):
            partial[e, :, 256 * n : 256 * n + 256] = plane_sum(e, 0, n, slice(None))

    def layer_one(e, h, rows=slice(None)):
        for n in (2 * h, 2 * h + 1):
            cols = slice(256 * n, 256 * n + 256)
            summed = partial[e, rows, cols] + plane_sum(e, 1, n, rows)
            first[rows, cols] = jnp.maximum(summed, 0.0).astype(BF16)

    def layers_two_three(e, start=0, size=tokens):
        rows = pl.ds(start, size)
        for n in range(2):
            w = jnp.concatenate(
                [w23[e % 2, e // 2, :, :, :, q, n, 0:64].reshape(16 * 64, 128) for q in range(2)], axis=1
            )
            summed = jnp.dot(first[rows], w, preferred_element_type=F32)
            second[rows, 256 * n : 256 * n + 256] = jnp.maximum(summed, 0.0).astype(BF16)
        w = jnp.concatenate(
            [w23[e % 2, e // 2, :, :, :, :, n, 64:80].reshape(32 * 16, 128) for n in range(2)], axis=1
        )
        for part in range(2):
            rows = pl.ds(start + part * (size // 2), size // 2)
            summed = jnp.dot(second[rows], w, preferred_element_type=F32)
            eo[0, e, rows] = jnp.maximum(summed, 0.0).astype(BF16)

    def compute(e, i):
        rows = pl.ds(i * chunk, chunk)
        for h in range(2):
            layer_one(e, h, rows)
        layers_two_three(e, i * chunk, chunk)
        push(eo_slots[e][i], eo.at[0, e, rows], eo.at[1, e, rows], task_peer)
        add_up(0, e, rows)

    def others(e):
        for i in range(3):
            arrived(eo_slots[e][i], eo.at[1, e, pl.ds(i * chunk, chunk)])
        add_up(1, e)

    def finish(i):
        rows = pl.ds(i * chunk, chunk)
        arrived(eo_slots[experts - 1][i], eo.at[1, experts - 1, rows])
        add_up(1, experts - 1, rows)
        for k in range(2):
            total = sum(weights[o, rows, 2 * e + k : 2 * e + k + 1] for o in range(2) for e in range(experts))
            mix = (numer[k, rows] / total).astype(BF16)
            tower = jnp.maximum(jnp.dot(mix, hidden_ref[k], preferred_element_type=F32), 0.0).astype(BF16)
            out_ref[k : k + 1, rows] = lax.dot_general(
                out_w_ref[k : k + 1, :], tower, (((1,), (1,)), ((), ())), preferred_element_type=F32
            )

    gates(0)
    quad(1)
    first_round(0)
    quad(2)
    first_round(1)
    first_round(2)
    first_done(0)
    push(gate_slot, gate_hbm, gate.at[1], task_peer)
    share(0, 0, (0,))
    quad(3)
    near(0, 0)
    first_done(1)
    near(1, 0)
    far(0, 0)
    gates(1)
    share(0, 0, (1, -1))
    first_round(3)
    share(1, 0, (0,))
    by_plane()
    far(1, 0)
    first_far(2)
    far_done(0, 0)
    z_done(0)
    share(0, 0, (2,))
    share_arrived(0, 0)
    share(1, 0, (1, -1))
    early(0, 0)
    far_done(1, 0)
    share(1, 0, (2,))
    early(0, 1)
    share(0, 1, (0,))
    first_done(2)
    share(2, 0, (0,))
    near(2, 0)
    first_far(3)
    share_arrived(1, 0)
    early(1, 0)
    early(1, 1)
    z_done(1)
    far(0, 1)
    share(0, 1, (1, -1))
    far(2, 0)
    first_done(3)
    share(1, 1, (0,))
    far(1, 1)
    near(3, 0)
    share(2, 0, (1, -1))
    share(1, 1, (1, -1))
    z_done(2)
    far_done(0, 1)
    share(0, 1, (2,))
    share_arrived(0, 1)
    compute(0, 0)
    far_done(2, 0)
    share(2, 0, (2,))
    compute(0, 1)
    far_done(1, 1)
    share(1, 1, (2,))
    compute(0, 2)
    share_arrived(2, 0)
    early(2, 0)
    z_done(3)
    share_arrived(1, 1)
    compute(1, 0)
    far(3, 0)
    compute(1, 1)
    early(2, 1)
    share(3, 0, (0,))
    share(2, 1, (0,))
    compute(1, 2)
    far(2, 1)
    share(2, 1, (1, -1))
    far_done(2, 1)
    share(2, 1, (2,))
    share(3, 0, (1, -1))
    share(3, 1, (0,))
    share_arrived(2, 1)
    far(3, 1)
    compute(2, 0)
    compute(2, 1)
    far_done(3, 0)
    share(3, 0, (2,))
    compute(2, 2)
    share(3, 1, (1, -1))
    share_arrived(3, 0)
    early(3, 0)
    far_done(3, 1)
    share(3, 1, (2,))
    early(3, 1)
    share_arrived(3, 1)
    compute(3, 0)
    compute(3, 1)
    compute(3, 2)
    others(0)
    others(2)
    others(1)
    for copy in sent[:-3]:
        copy.wait_send()
    for i in range(3):
        finish(i)
    for copy in sent[-3:]:
        copy.wait_send()


def per_device(pooled, gate_weight, w_first, w_second, w_third, tower_hidden, tower_out):
    tokens, width = pooled.shape
    experts = w_first.shape[0]
    any_, vmem = pl.BlockSpec(memory_space=pl.ANY), pl.BlockSpec(memory_space=pltpu.VMEM)
    slots = 300
    return pl.pallas_call(
        kernel,
        out_shape=jax.ShapeDtypeStruct((2, tokens), F32),
        in_specs=[any_] * 5 + [vmem, vmem],
        out_specs=vmem,
        scratch_shapes=[
            pltpu.VMEM((52, experts, 1024), BF16),
            pltpu.VMEM((experts, 16, 512), BF16),
            pltpu.VMEM((experts, 8, 256), BF16),
            pltpu.VMEM((QUAD, experts, BLOCK, 256), BF16),
            pltpu.VMEM((QUAD, experts, BLOCK, 256), BF16),
            pltpu.VMEM((experts, 4, 2, 2, 208, 1024), BF16),
            pltpu.VMEM((2, 2, 4, 2, 2, 2, 2, 80, 128), BF16),
            pltpu.VMEM((tokens, width), BF16),
            pltpu.VMEM((2, experts, 4, width), BF16),
            pltpu.VMEM((tokens, 1024), BF16),
            pltpu.VMEM((tokens, 512), BF16),
            pltpu.VMEM((experts, tokens, 1024), F32),
            pltpu.VMEM((2, experts, tokens, 256), BF16),
            pltpu.VMEM((2, tokens, 256), F32),
            pltpu.VMEM((2, tokens, 2 * experts), F32),
            pltpu.SemaphoreType.DMA((slots,)),
            pltpu.SemaphoreType.DMA((slots,)),
            pltpu.SemaphoreType.DMA((6,)),
        ],
        compiler_params=pltpu.CompilerParams(
            collective_id=0, has_side_effects=True, vmem_limit_bytes=67_000_000
        ),
    )(
        pooled, gate_weight.transpose(1, 2, 0), w_first.transpose(1, 0, 2), w_second, w_third, tower_hidden, tower_out
    ).T


def solution(mesh):
    torus = Mesh(mesh.devices.reshape(mesh.shape["task"], 4, 2, 4, 2), AXES)
    return jax.shard_map(
        per_device,
        mesh=torus,
        in_specs=(
            P(BATCH, None),
            P(None, "task", None),
            P("task", BATCH, None),
            P("task", BATCH, None),
            P("task", BATCH, None),
            P("task", None, None),
            P("task", None),
        ),
        out_specs=P(BATCH, "task"),
        check_vma=False,
    )
```

```python
import functools

import jax
import jax.numpy as jnp
from jax import lax
from jax.experimental import pallas as pl
from jax.experimental.pallas import tpu as pltpu
from jax.sharding import Mesh
from jax.sharding import PartitionSpec as P

AXES = ("task", "batch_0", "batch_1", "batch_2", "batch_3")
BATCH = AXES[1:]
MESH = pl.DeviceIdType.MESH
BF16 = jnp.bfloat16
F32 = jnp.float32

W1_ROWS, W2_ROWS, W3_ROWS = 52, 8, 4
QUAD = 4
BLOCK = W1_ROWS + W2_ROWS + W3_ROWS


def one_hot(rows, source):
    row = lax.broadcasted_iota(jnp.int32, (rows, QUAD * BLOCK), 0)
    column = lax.broadcasted_iota(jnp.int32, (rows, QUAD * BLOCK), 1)
    return jnp.where(source(row) == column, 1.0, 0.0).astype(BF16)


def picked(selector, values):
    return jnp.dot(selector, values, preferred_element_type=F32).astype(BF16)


def kernel(
    pooled_hbm, gate_hbm, first_hbm, second_hbm, third_hbm, hidden_ref, out_w_ref, out_ref,
    raw1, raw2, raw3, block, staged, w1, w23, pooled, gate, first, second, partial, eo, numer, weights, send_sem, recv_sem, local_sem,
):
    t, y, zh, x, c = (lax.axis_index(a) for a in AXES)
    xp, xq = x // 2, lax.rem(x, 2)
    j = 2 * xq + c
    tq = jnp.where(zh == 1, t, 1 - t)
    experts = w1.shape[0]
    tokens = pooled.shape[0]

    def at(pos, k):
        return lax.rem(pos + (k + 4), 4)

    core_peer = (t, y, zh, x, 1 - c)
    z_peer = (1 - t, y, 1 - zh, x, c)
    task_peer = (1 - t, y, zh, x, c)
    x_dev = lambda k: (t, y, zh, at(x, k), c)
    y_dev = lambda k: (t, at(y, k), zh, x, c)

    def quad_dev(d):
        dx, dc = d // 2, d % 2
        return (tq, y, zh, 2 * xp + (1 - xq if dx else xq), 1 - c if dc else c)

    used = [0]
    sent = []

    def slot():
        used[0] += 1
        return used[0] - 1

    def push(i, src, dst, device):
        copy = pltpu.make_async_remote_copy(
            src_ref=src, dst_ref=dst, send_sem=send_sem.at[i], recv_sem=recv_sem.at[i],
            device_id=device, device_id_type=MESH,
        )
        copy.start()
        sent.append(copy)

    def arrived(i, dst):
        pltpu.make_async_remote_copy(
            src_ref=dst, dst_ref=dst, send_sem=send_sem.at[i], recv_sem=recv_sem.at[i],
            device_id=core_peer, device_id_type=MESH,
        ).wait_recv()

    half = tokens // 2
    shards = [
        pltpu.make_async_copy(src, dst, local_sem.at[i])
        for i, (src, dst) in enumerate([(first_hbm, raw1), (second_hbm, raw2), (third_hbm, raw3)])
    ]
    loads = [
        pltpu.make_async_copy(pooled_hbm.at[pl.ds(k * half, half)], pooled.at[pl.ds(k * half, half)], local_sem.at[3 + k])
        for k in range(2)
    ]
    loads.append(pltpu.make_async_copy(gate_hbm, gate.at[0], local_sem.at[5]))
    for load in shards + loads:
        load.start()

    barrier = pltpu.get_barrier_semaphore()
    peers = [x_dev(1), x_dev(-1), x_dev(2), y_dev(1), y_dev(-1), y_dev(2), z_peer, core_peer, task_peer] + [quad_dev(d) for d in range(1, QUAD)]
    for device in peers:
        pl.semaphore_signal(barrier, inc=1, device_id=device, device_id_type=MESH)

    for load in shards:
        load.wait()

    def place(rows, columns, source):
        row = lax.broadcasted_iota(jnp.int32, (rows, columns), 0)
        column = lax.broadcasted_iota(jnp.int32, (rows, columns), 1)
        return jnp.where(source(row) == column, 1.0, 0.0).astype(BF16)

    def band(row, start, size, source):
        return jnp.where((row >= start) & (row < start + size), source, -1)

    def build(e):
        put1 = place(BLOCK, experts * W1_ROWS, lambda r: band(r, 0, W1_ROWS, experts * r + e))
        rows1 = jnp.dot(put1, raw1[...].reshape(experts * W1_ROWS, 1024), preferred_element_type=F32)
        rows2, rows3 = [], []
        for side in range(2):
            put2 = place(BLOCK, 16, lambda r: band(r, W1_ROWS, W2_ROWS, r - W1_ROWS + W2_ROWS * side))
            put3 = place(BLOCK, 8, lambda r: band(r, W1_ROWS + W2_ROWS, W3_ROWS, r - W1_ROWS - W2_ROWS + W3_ROWS * side))
            rows2.append(jnp.dot(put2, raw2[e], preferred_element_type=F32))
            rows3.append(jnp.dot(put3, raw3[e], preferred_element_type=F32))
        for member in range(QUAD):
            q, n = member // 2, member % 2
            for side in range(2):
                col1, col2, col3 = 512 * n + 256 * side + 128 * q, 256 * n + 128 * q, 128 * n
                both = rows1[:, col1 : col1 + 128] + rows2[side][:, col2 : col2 + 128] + rows3[side][:, col3 : col3 + 128]
                block[member, e, :, 128 * side : 128 * side + 128] = both.astype(BF16)

    build(0)
    pl.semaphore_wait(barrier, len(peers))

    def member(d):
        return 2 * ((1 - xq) if d // 2 else xq) + ((1 - c) if d % 2 else c)

    quad_slots = [[slot() for _ in range(QUAD)] for _ in range(experts)]
    own_far = [
        pltpu.make_async_remote_copy(
            src_ref=block.at[j, e], dst_ref=staged.at[j, e], send_sem=send_sem.at[quad_slots[e][0]],
            recv_sem=recv_sem.at[quad_slots[e][0]], device_id=task_peer, device_id_type=MESH,
        )
        for e in range(experts)
    ]

    def quad(e):
        for d in range(1, QUAD):
            push(quad_slots[e][d], block.at[member(d), e], staged.at[j, e], quad_dev(d))

        @pl.when(zh == 0)
        def _():
            own_far[e].start()

        @pl.when(zh == 1)
        def _():
            staged[j, e] = block[j, e]

    quad(0)
    for e in range(1, experts):
        build(e)
    gate_slot = slot()

    def w1_source(r):
        return r + (BLOCK - W1_ROWS) * (
            (r >= W1_ROWS).astype(jnp.int32) + (r >= 2 * W1_ROWS).astype(jnp.int32) + (r >= 3 * W1_ROWS).astype(jnp.int32)
        )

    def half_source(r, unit, side, base):
        member, within = r // (2 * unit), lax.rem(r, 2 * unit)
        return jnp.where(within // unit == side, BLOCK * member + base + lax.rem(within, unit), -1)

    pick1 = one_hot(QUAD * W1_ROWS, w1_source)
    pick2 = [one_hot(QUAD * 16, lambda r, s=s: half_source(r, W2_ROWS, s, W1_ROWS)) for s in range(2)]
    pick3 = [
        one_hot(16, lambda r, s=s: jnp.where(
            half_source(r, W3_ROWS, s, W1_ROWS + W2_ROWS) >= 0,
            half_source(r, W3_ROWS, s, W1_ROWS + W2_ROWS) + 2 * BLOCK * xq, -1))
        for s in range(2)
    ]
    col0 = pl.multiple_of(512 * c, 128)

    def w1_cols(h, xq_):
        return pl.ds(pl.multiple_of(512 * c + 256 * h + 128 * xq_, 128), 128)

    def pack(e):
        for d in range(1, QUAD):
            arrived(quad_slots[e][d], staged.at[member(d), e])

        @pl.when(zh == 0)
        def _():
            own_far[e].wait()

        rows = staged[:, e].reshape(QUAD * BLOCK, 256)
        w1_part = picked(pick1, rows)
        w1[e, y, zh, xp, :, w1_cols(0, xq)] = w1_part[:, :128]
        w1[e, y, zh, xp, :, w1_cols(1, xq)] = w1_part[:, 128:]
        w23[e % 2, e // 2, y, zh, xp, xq, c, 0:64] = picked(
            jnp.concatenate(pick2, axis=1), jnp.concatenate([rows[:, :128], rows[:, 128:]], axis=0)
        )
        w23[e % 2, e // 2, y, zh, xp, xq, c, 64:80] = picked(
            jnp.concatenate(pick3, axis=1), jnp.concatenate([rows[:, :128], rows[:, 128:]], axis=0)
        )

    def plane(o):
        return zh if o == 0 else 1 - zh

    def a1(e, k):
        x_ = at(x, k)
        return w1.at[e, y, zh, x_ // 2, :, w1_cols(0, lax.rem(x_, 2))]

    def b1(e, k):
        return w1.at[e, at(y, k), zh, xp, :, w1_cols(1, xq)]

    def c1(e, k):
        if e % 2 == 0:
            x_ = at(x, k)
            return w23.at[0, e // 2, y, zh, x_ // 2, lax.rem(x_, 2), c]
        return w23.at[1, e // 2, at(y, k), zh, xp, xq, c]

    def a2(e, k, o, core, rows=slice(None)):
        return w1.at[e, at(y, k), plane(o), rows, :, pl.ds(pl.multiple_of(512 * core, 128), 256)]

    def b2(e, k, o, core, rows=slice(None)):
        x_ = at(x, k)
        cols = pl.ds(pl.multiple_of(512 * core + 256 + 128 * lax.rem(x_, 2), 128), 128)
        return w1.at[e, rows, plane(o), x_ // 2, :, cols]

    def c2(e, k, o, core, rows=slice(None)):
        if e % 2 == 0:
            return w23.at[0, e // 2, at(y, k), plane(o), rows, :, core]
        x_ = at(x, k)
        return w23.at[1, e // 2, rows, plane(o), x_ // 2, lax.rem(x_, 2), core]

    class Ring:
        def __init__(self, device, part, ways, direct=False):
            self.device, self.part, self.ways, self.direct = device, part, ways, direct
            self.slots = {k: slot() for k in (1, -1)}
            self.far_slots = {k: slot() for k in ways}

        def near(self):
            for k in (1, -1):
                push(self.slots[k], self.part(0), self.part(0), self.device(k))
            if self.direct:
                for k in self.ways:
                    push(self.far_slots[k], self.part(0), self.part(0), self.device(2))

        def near_arrived(self):
            for k in (1, -1):
                arrived(self.slots[k], self.part(-k))

        def far(self):
            self.near_arrived()
            for k, half in self.ways.items():
                push(self.far_slots[k], half(-k), half(-k), self.device(k))

        def far_arrived(self):
            for k, half in self.ways.items():
                arrived(self.far_slots[k], half(2))

    one, two, z_slots, shared = [], [], [], []
    for e in range(experts):
        x_first, y_first = (x_dev, y_dev), (y_dev, x_dev)
        parts = [
            (x_first, lambda k, e=e: a1(e, k), functools.partial(a2, e), 2),
            (y_first, lambda k, e=e: b1(e, k), functools.partial(b2, e), 4),
            (x_first if e % 2 == 0 else y_first, lambda k, e=e: c1(e, k), functools.partial(c2, e), 2 if e % 2 == 0 else 4),
        ]
        one.append([Ring(d[0], p1, {(1 if (e + i) % 2 == 0 else -1): p1}, e < 2) for i, (d, p1, _, _) in enumerate(parts)])
        two.append([
            [
                Ring(d[1], lambda k, p2=p2, o=o: p2(k, o, c), {
                    1: lambda k, p2=p2, o=o, n=n: p2(k, o, c, pl.ds(0, n // 2)),
                    -1: lambda k, p2=p2, o=o, n=n: p2(k, o, c, pl.ds(n // 2, n // 2)),
                })
                for d, _, p2, n in parts
            ]
            for o in range(2)
        ])
        z_slots.append([slot() for _ in parts])
        shared.append([(p2, {(k, o): slot() for k in (0, 1, -1, 2) for o in range(2)}) for _, _, p2, _ in parts])

    def share(e, o, which):
        for part, slots in shared[e]:
            for k in which:
                push(slots[k, o], part(k, o, c), part(k, o, c), core_peer)

    def share_arrived(e, o):
        for part, slots in shared[e]:
            for k in (0, 1, -1, 2):
                arrived(slots[k, o], part(k, o, 1 - c))

    def each(rings, step):
        for ring in rings:
            getattr(ring, step)()

    def first_round(e):
        pack(e)
        each(one[e], "near")

    def first_far(e):
        each(one[e], "far")

    def first_done(e):
        if e < 2:
            each(one[e], "near_arrived")
        each(one[e], "far_arrived")
        for (part, _), i in zip(shared[e], z_slots[e]):
            push(i, part(0, 0, c), part(0, 0, c), z_peer)

    def near(e, o):
        each(two[e][o], "near")

    def z_done(e):
        for (part, _), i in zip(shared[e], z_slots[e]):
            arrived(i, part(0, 1, c))
        near(e, 1)

    far_by_z = {e: [slot() for _ in range(3)] for e in (2,)}

    def far(e, o):
        each(two[e][o], "near_arrived" if o == 1 and e in far_by_z else "far")

    def far_done(e, o):
        if o == 1 and e in far_by_z:
            for (part, _), i in zip(shared[e], far_by_z[e]):
                arrived(i, part(2, 1, c))
        else:
            each(two[e][o], "far_arrived")
        if o == 0 and e in far_by_z:
            for (part, _), i in zip(shared[e], far_by_z[e]):
                push(i, part(2, 0, c), part(2, 0, c), z_peer)

    def gates(o):
        if o == 0:
            for load in loads:
                load.wait()
            numer[...] = jnp.zeros_like(numer)
        else:
            arrived(gate_slot, gate.at[1])
        side = jnp.where(zh == 1, o, 1 - o)
        g = gate[o].reshape(4 * experts, pooled.shape[1])
        for part in range(2):
            rows = pl.ds(part * half, half)
            logits = lax.dot_general(pooled[rows], g, (((1,), (1,)), ((), ())), preferred_element_type=F32)
            for e in range(experts):
                own = jnp.where(t == 0, logits[:, 4 * e : 4 * e + 2], logits[:, 4 * e + 2 : 4 * e + 4])
                weights[side, rows, 2 * e : 2 * e + 2] = jnp.exp(own)

    chunk = tokens // 3
    even = [(i * chunk, chunk) for i in range(3)]
    short = chunk // 2
    chunks = [even] * (experts - 1) + [[(0, short), (short, chunk), (short + chunk, chunk), (short + 2 * chunk, short)]]
    eo_slots = [[slot() for _ in pieces] for pieces in chunks]
    assert used[0] <= send_sem.shape[0], used[0]

    def add_up(o, e, rows=slice(None)):
        values = eo[o, e, rows].astype(F32)
        for k in range(2):
            numer[k, rows] += weights[o, rows, 2 * e + k : 2 * e + k + 1] * values

    def by_plane():
        run, rows_each = 2 * 208, tokens // 12

        @pl.loop(0, 12)
        def _(i):
            rows = pl.ds(pl.multiple_of(i * rows_each, rows_each), rows_each)
            values = pooled[rows]
            pooled[rows] = jnp.concatenate(
                [values[:, (2 * n + p) * run : (2 * n + p + 1) * run] for p in range(2) for n in range(4)], axis=1
            )

    def plane_sum(e, o, n, rows):
        p = plane(o)
        depth = 8 * 208
        w = w1[e, :, p, :, :, 256 * n : 256 * n + 256].reshape(depth, 256)
        return jnp.dot(pooled[rows, pl.ds(pl.multiple_of(p * depth, 128), depth)], w, preferred_element_type=F32)

    def early(e, h):
        for n in (2 * h, 2 * h + 1):
            partial[e, :, 256 * n : 256 * n + 256] = plane_sum(e, 0, n, slice(None))

    def layer_one(e, h, rows=slice(None)):
        for n in (2 * h, 2 * h + 1):
            cols = slice(256 * n, 256 * n + 256)
            summed = partial[e, rows, cols] + plane_sum(e, 1, n, rows)
            first[rows, cols] = jnp.maximum(summed, 0.0).astype(BF16)

    def layers_two_three(e, start=0, size=tokens):
        rows = pl.ds(start, size)
        for n in range(2):
            w = jnp.concatenate(
                [w23[e % 2, e // 2, :, :, :, q, n, 0:64].reshape(16 * 64, 128) for q in range(2)], axis=1
            )
            summed = jnp.dot(first[rows], w, preferred_element_type=F32)
            second[rows, 256 * n : 256 * n + 256] = jnp.maximum(summed, 0.0).astype(BF16)
        w = jnp.concatenate(
            [w23[e % 2, e // 2, :, :, :, :, n, 64:80].reshape(32 * 16, 128) for n in range(2)], axis=1
        )
        for part in range(2):
            rows = pl.ds(start + part * (size // 2), size // 2)
            summed = jnp.dot(second[rows], w, preferred_element_type=F32)
            eo[0, e, rows] = jnp.maximum(summed, 0.0).astype(BF16)

    def compute(e, i):
        start, size = chunks[e][i]
        rows = pl.ds(start, size)
        for h in range(2):
            layer_one(e, h, rows)
        layers_two_three(e, start, size)
        push(eo_slots[e][i], eo.at[0, e, rows], eo.at[1, e, rows], task_peer)
        add_up(0, e, rows)

    def others(e):
        for i in range(3):
            arrived(eo_slots[e][i], eo.at[1, e, pl.ds(i * chunk, chunk)])
        add_up(1, e)

    def finish(i):
        rows = pl.ds(*chunks[experts - 1][i])
        arrived(eo_slots[experts - 1][i], eo.at[1, experts - 1, rows])
        add_up(1, experts - 1, rows)
        for k in range(2):
            total = sum(weights[o, rows, 2 * e + k : 2 * e + k + 1] for o in range(2) for e in range(experts))
            mix = (numer[k, rows] / total).astype(BF16)
            tower = jnp.maximum(jnp.dot(mix, hidden_ref[k], preferred_element_type=F32), 0.0).astype(BF16)
            out_ref[k : k + 1, rows] = lax.dot_general(
                out_w_ref[k : k + 1, :], tower, (((1,), (1,)), ((), ())), preferred_element_type=F32
            )

    gates(0)
    quad(1)
    first_round(0)
    quad(2)
    first_round(1)
    first_round(2)
    first_done(0)
    push(gate_slot, gate_hbm, gate.at[1], task_peer)
    share(0, 0, (0,))
    quad(3)
    near(0, 0)
    first_done(1)
    near(1, 0)
    far(0, 0)
    gates(1)
    share(0, 0, (1, -1))
    first_round(3)
    share(1, 0, (0,))
    by_plane()
    far(1, 0)
    first_far(2)
    far_done(0, 0)
    z_done(0)
    share(0, 0, (2,))
    share_arrived(0, 0)
    share(1, 0, (1, -1))
    early(0, 0)
    far_done(1, 0)
    share(1, 0, (2,))
    early(0, 1)
    share(0, 1, (0,))
    first_done(2)
    share(2, 0, (0,))
    near(2, 0)
    first_far(3)
    share_arrived(1, 0)
    early(1, 0)
    early(1, 1)
    z_done(1)
    far(0, 1)
    share(0, 1, (1, -1))
    far(2, 0)
    first_done(3)
    share(1, 1, (0,))
    far(1, 1)
    near(3, 0)
    share(2, 0, (1, -1))
    share(1, 1, (1, -1))
    z_done(2)
    far_done(0, 1)
    share(0, 1, (2,))
    share_arrived(0, 1)
    compute(0, 0)
    far_done(2, 0)
    share(2, 0, (2,))
    compute(0, 1)
    far_done(1, 1)
    share(1, 1, (2,))
    compute(0, 2)
    share_arrived(2, 0)
    early(2, 0)
    z_done(3)
    share_arrived(1, 1)
    compute(1, 0)
    far(3, 0)
    compute(1, 1)
    early(2, 1)
    share(3, 0, (0,))
    share(2, 1, (0,))
    compute(1, 2)
    far(2, 1)
    share(2, 1, (1, -1))
    far_done(2, 1)
    share(2, 1, (2,))
    share(3, 0, (1, -1))
    share(3, 1, (0,))
    share_arrived(2, 1)
    far(3, 1)
    compute(2, 0)
    compute(2, 1)
    far_done(3, 0)
    share(3, 0, (2,))
    compute(2, 2)
    share(3, 1, (1, -1))
    share_arrived(3, 0)
    early(3, 0)
    far_done(3, 1)
    share(3, 1, (2,))
    early(3, 1)
    share_arrived(3, 1)
    compute(3, 0)
    compute(3, 1)
    compute(3, 2)
    compute(3, 3)
    others(0)
    others(2)
    others(1)
    for copy in sent[:-4]:
        copy.wait_send()
    for i in range(4):
        finish(i)
    for copy in sent[-4:]:
        copy.wait_send()


def per_device(pooled, gate_weight, w_first, w_second, w_third, tower_hidden, tower_out):
    tokens, width = pooled.shape
    experts = w_first.shape[0]
    any_, vmem = pl.BlockSpec(memory_space=pl.ANY), pl.BlockSpec(memory_space=pltpu.VMEM)
    slots = 300
    return pl.pallas_call(
        kernel,
        out_shape=jax.ShapeDtypeStruct((2, tokens), F32),
        in_specs=[any_] * 5 + [vmem, vmem],
        out_specs=vmem,
        scratch_shapes=[
            pltpu.VMEM((52, experts, 1024), BF16),
            pltpu.VMEM((experts, 16, 512), BF16),
            pltpu.VMEM((experts, 8, 256), BF16),
            pltpu.VMEM((QUAD, experts, BLOCK, 256), BF16),
            pltpu.VMEM((QUAD, experts, BLOCK, 256), BF16),
            pltpu.VMEM((experts, 4, 2, 2, 208, 1024), BF16),
            pltpu.VMEM((2, 2, 4, 2, 2, 2, 2, 80, 128), BF16),
            pltpu.VMEM((tokens, width), BF16),
            pltpu.VMEM((2, experts, 4, width), BF16),
            pltpu.VMEM((tokens, 1024), BF16),
            pltpu.VMEM((tokens, 512), BF16),
            pltpu.VMEM((experts, tokens, 1024), F32),
            pltpu.VMEM((2, experts, tokens, 256), BF16),
            pltpu.VMEM((2, tokens, 256), F32),
            pltpu.VMEM((2, tokens, 2 * experts), F32),
            pltpu.SemaphoreType.DMA((slots,)),
            pltpu.SemaphoreType.DMA((slots,)),
            pltpu.SemaphoreType.DMA((6,)),
        ],
        compiler_params=pltpu.CompilerParams(
            collective_id=0, has_side_effects=True, vmem_limit_bytes=67_000_000
        ),
    )(
        pooled, gate_weight.transpose(1, 2, 0), w_first.transpose(1, 0, 2), w_second, w_third, tower_hidden, tower_out
    ).T


def solution(mesh):
    torus = Mesh(mesh.devices.reshape(mesh.shape["task"], 4, 2, 4, 2), AXES)
    return jax.shard_map(
        per_device,
        mesh=torus,
        in_specs=(
            P(BATCH, None),
            P(None, "task", None),
            P("task", BATCH, None),
            P("task", BATCH, None),
            P("task", BATCH, None),
            P("task", None, None),
            P("task", None),
        ),
        out_specs=P(BATCH, "task"),
        check_vma=False,
    )
```
